32 devices in a mesh: tok: 4 (over y, x), din: 4 (over z), dout: 2 (over core).
Axes of the slice: x: 2, y: 2, z: 4, core: 2. Of those that a mesh axis runs over, the one named last changes fastest.
Arguments:
- inputs: bfloat16 [1024, 7168], P(('tok', 'dout'), 'din'), may hold values from -6 to 6
- out_grad: bfloat16 [1024, 9216], P(('tok', 'din'), 'dout'), may hold values from -0.1875 to 0.1875
Outputs:
- weight_grad: bfloat16 [7168, 9216], P(('din', 'tok'), 'dout')
The draws below stay inside these ranges and needn't reach their ends.
All inputs are finite; a program needn't handle non-finite values.
Results may differ from the reference program's by a relative error of at most 0.014.
Values may be sent and summed in bfloat16 or wider, within the bound.
A program may use at most 64 MiB of HBM per device.

```python
import jax
import jax.numpy as jnp
from jax import lax

D = 7168
F = 9216
GROUP_ROWS = 256
TOKENS = 1024
N_TOK = 4


def spiked(drawn, rng, source, target, shards_of, factor):
    def block_of(axis_at):
        return (jnp.arange(drawn.shape[axis_at]) // (drawn.shape[axis_at] // shards_of)).reshape((-1,) + (1,) * (drawn.ndim - 1 - axis_at))

    near = jax.random.permutation(rng, shards_of)[block_of(target)]
    other_side = (block_of(target) + shards_of // 2) % shards_of
    return jnp.where((block_of(source) == near) | (block_of(source) == other_side), factor * drawn, drawn)


def block_levels(key, extent, split, smallest, largest):
    def one(position, parts):
        heights = jax.random.uniform(jax.random.fold_in(jax.random.fold_in(key, 6), position), (parts,), jnp.float32, smallest / len(split), largest / len(split))
        return jnp.repeat(jnp.exp(heights), extent[position] // parts).reshape((-1,) + (1,) * (len(extent) - position - 1))

    loudness = one(*split[0])
    for cut in split[1:]:
        loudness = loudness * one(*cut)
    return loudness


def gaussian(key, extent, scale, limit, split=(), kind=jnp.bfloat16):
    drawn = scale * jax.random.normal(key, extent, jnp.float32)
    if split:
        drawn = drawn * block_levels(key, extent, split, -0.22, 0.18)
    return jnp.clip(drawn, -limit, limit).astype(kind)


def noise_with(stream_key, dims, spread, reach, cuts, heavy, kind=jnp.bfloat16):
    result = spread * jax.random.normal(stream_key, dims, jnp.float32)
    if cuts:
        result = result * block_levels(stream_key, dims, cuts, -0.22, 0.18)
    return jnp.clip(spiked(result, jax.random.fold_in(stream_key, 3), *heavy), -reach, reach).astype(kind)


def setup_inputs(seed: int = 0) -> dict:
    seeds = jax.random.split(jax.random.key(seed), 3)
    inputs = noise_with(seeds[0], (TOKENS, D), 1.0, 6.0, ((0, 8), (1, 4)), (0, 1, 8, 2.0))
    out_grad = gaussian(seeds[1], (TOKENS, F), TOKENS ** -0.5, 0.1875, ((0, 16), (1, 2)))
    return {"inputs": inputs, "out_grad": out_grad}


def reference(inputs, out_grad):
    def add_group(total, index):
        start = (index * GROUP_ROWS).astype(jnp.int32)
        rows_in = lax.dynamic_slice_in_dim(inputs, start, GROUP_ROWS, 0)
        rows_grad = lax.dynamic_slice_in_dim(out_grad, start, GROUP_ROWS, 0)
        term = lax.dot_general(rows_in, rows_grad, (((0,), (0,)), ((), ())), preferred_element_type=jnp.float32)
        return total + term.astype(jnp.bfloat16).astype(jnp.float32), None

    total = jnp.zeros((D, F), jnp.float32)
    total, _ = lax.scan(add_group, total, jnp.arange(N_TOK, dtype=jnp.int32))
    return total.astype(jnp.bfloat16)
```

```python
import functools

import jax
import jax.numpy as jnp
from jax import lax
from jax.experimental import pallas as pl
from jax.experimental.pallas import tpu as pltpu
from jax.sharding import PartitionSpec as P

MESH = pl.DeviceIdType.MESH
LANES = 128
STRIPS = 2
WIDE = STRIPS * LANES


def scattered(inputs, out_grad):
    gathered = lax.all_gather(inputs, "dout", axis=0, tiled=True)
    partial_term = lax.dot_general(
        gathered,
        lax.all_gather(out_grad, "din", axis=0, tiled=True),
        (((0,), (0,)), ((), ())),
        preferred_element_type=jnp.float32,
    )
    return lax.psum_scatter(
        partial_term.astype(jnp.bfloat16), "tok", scatter_dimension=0, tiled=True
    )


def plan(columns):
    total = columns // WIDE
    whole = 2 - total % 2
    split = (total - whole) // 2
    places = [(split * (g + 1)) // whole + g if g < whole - 1 else split + g for g in range(whole)]
    return split, whole, places


def kernel(sizes, a_ref, g_ref, o_ref, give, held, full, away, windows, left, ship,
           give_load, own_load, full_load, a_load,
           swap_send, swap_recv, fx_send, fx_recv, fy_send, fy_recv,
           a_send, a_recv, p_send, p_recv,
           z_send, z_recv, y_send, y_recv, out_send, out_recv):
    depth, split, whole, places, rows = sizes
    units = split + whole
    t, z, core = lax.axis_index("tok"), lax.axis_index("din"), lax.axis_index("dout")
    y, x = t // 2, t % 2
    near_x = (y * 2 + (1 - x), z, core)
    near_y = ((1 - y) * 2 + x, z, core)
    partner = (t, z, 1 - core)
    half = split * WIDE
    pair = 2 * rows

    def columns_of(side, c):
        return pl.multiple_of(side * half + c * WIDE, WIDE)

    def strip(start, j):
        return g_ref.at[:, pl.ds(pl.multiple_of(start + j * LANES, LANES), LANES)]

    def give_in(c, j):
        return pltpu.make_async_copy(strip(columns_of(1 - x, c), j), give.at[c, j], give_load.at[c, j])

    def own_in(c, j):
        return pltpu.make_async_copy(strip(columns_of(x, c), j), held.at[c, y, x, z, j], own_load.at[c, j])

    def full_in(g, j):
        return pltpu.make_async_copy(
            strip(2 * half + g * WIDE, j), full.at[g, y, x, z, j], full_load.at[g, j]
        )

    def a_in(i):
        src = a_ref.at[:, pl.ds(pl.multiple_of((y if i == 0 else 1 - y) * pair, LANES), pair)]
        return pltpu.make_async_copy(src, windows.at[y, x, core] if i == 0 else away, a_load.at[i])

    def load(c, carry):
        for j in range(STRIPS):
            give_in(c, j).start()
            own_in(c, j).start()
        return carry

    load(0, 0)
    a_in(0).start()
    a_in(1).start()
    lax.fori_loop(1, split, load, 0)
    for g in range(whole):
        for j in range(STRIPS):
            full_in(g, j).start()

    barrier = pltpu.get_barrier_semaphore()
    for other in (near_x, near_y, partner):
        pl.semaphore_signal(barrier, inc=1, device_id=other, device_id_type=MESH)

    @pl.when(z > 0)
    def _():
        pl.semaphore_signal(barrier, inc=1, device_id=(t, z - 1, core), device_id_type=MESH)

    @pl.when(z < depth - 1)
    def _():
        pl.semaphore_signal(barrier, inc=1, device_id=(t, z + 1, core), device_id_type=MESH)

    pl.semaphore_wait(barrier, 3 + jnp.where(z > 0, 1, 0) + jnp.where(z < depth - 1, 1, 0))

    def remote(src, dst, send, recv, device):
        return pltpu.make_async_remote_copy(
            src_ref=src, dst_ref=dst, send_sem=send, recv_sem=recv,
            device_id=device, device_id_type=MESH,
        )

    def swap(c):
        return remote(give.at[c], held.at[c, y, x, z], swap_send.at[c], swap_recv.at[c], near_x)

    def swap_wait(c):
        ref = held.at[c, y, 1 - x, z]
        remote(ref, ref, swap_send.at[c], swap_recv.at[c], near_x).wait_recv()

    def full_x(g, side):
        ref = full.at[g, y, side, z]
        return remote(ref, ref, fx_send.at[g], fx_recv.at[g], near_x)

    def full_y(g, row):
        ref = full.at[g, row, :, z]
        return remote(ref, ref, fy_send.at[g], fy_recv.at[g], near_y)

    def a_out(i):
        src = (windows.at[y, x, core], away, windows.at[1 - y, x, core])[i]
        dst = (windows.at[y, x, core], windows.at[y, x, core], windows.at[1 - y, x, core])[i]
        return remote(src, dst, a_send.at[i], a_recv.at[i], near_y if i == 1 else near_x)

    def a_wait(i):
        ref = (windows.at[y, 1 - x, core], windows.at[1 - y, x, core], windows.at[1 - y, 1 - x, core])[i]
        remote(ref, ref, a_send.at[i], a_recv.at[i], near_y if i == 1 else near_x).wait_recv()

    def group(i):
        return ((y, 1 - x), (1 - y, x), (1 - y, 1 - x), (y, x))[i]

    def over(i, side):
        yy, xx = group(i)
        ref = windows.at[yy, xx, side]
        return remote(ref, ref, p_send.at[i], p_recv.at[i], partner)

    def line(u, ref, source, up):
        return remote(
            ref, ref, z_send.at[u, source, up], z_recv.at[u, source],
            (t, z + 1 if up else z - 1, core),
        )

    def to_y(u, c, source, row):
        ref = held.at[c, row, :, source]
        return remote(ref, ref, y_send.at[u, source], y_recv.at[u, source], near_y)

    def by_kind(u, on_split, on_whole):
        is_whole = functools.reduce(jnp.logical_or, [u == p for p in places])
        before = sum(jnp.where(u > p, 1, 0) for p in places)

        @pl.when(jnp.logical_not(is_whole))
        def _():
            on_split(u - before)

        @pl.when(is_whole)
        def _():
            on_whole(before)

    def both_ways(u, ref):
        @pl.when(z < depth - 1)
        def _():
            line(u, ref, z, 1).start()

        @pl.when(z > 0)
        def _():
            line(u, ref, z, 0).start()

    def start_own(u):
        def on_split(c):
            for j in range(STRIPS):
                own_in(c, j).wait()
            swap_wait(c)
            both_ways(u, held.at[c, y, :, z])
            to_y(u, c, z, y).start()

        def on_whole(g):
            full_y(g, 1 - y).wait_recv()
            both_ways(u, full.at[g, :, :, z])

        by_kind(u, on_split, on_whole)

    def pass_on(u, hop):
        def on(of, then):
            @pl.when(z - hop >= 0)
            def _():
                ref = of(z - hop)
                line(u, ref, z - hop, 0).wait_recv()

                @pl.when(z < depth - 1)
                def _():
                    line(u, ref, z - hop, 1).start()

                then(z - hop)

            @pl.when(z + hop < depth)
            def _():
                ref = of(z + hop)
                line(u, ref, z + hop, 1).wait_recv()

                @pl.when(z > 0)
                def _():
                    line(u, ref, z + hop, 0).start()

                then(z + hop)

        by_kind(
            u,
            lambda c: on(lambda s: held.at[c, y, :, s], lambda s: to_y(u, c, s, y).start()),
            lambda g: on(lambda s: full.at[g, :, :, s], lambda s: None),
        )

    def out(c, side):
        dst = o_ref.at[:, pl.ds(columns_of(side, c), WIDE)]
        return remote(ship.at[c], dst, out_send.at[c], out_recv.at[c], near_x)

    def term(side, block):
        wide = jnp.concatenate([block[:, :, :, j].reshape(-1, LANES) for j in range(STRIPS)], axis=1)
        return jnp.dot(left[side], wide, preferred_element_type=jnp.float32).astype(o_ref.dtype)

    def multiply(u):
        def on_split(c):
            for source in range(depth):
                to_y(u, c, source, 1 - y).wait_recv()
            ship[c] = term(1 - x, held.at[c])
            o_ref[:, pl.ds(columns_of(x, c), WIDE)] = term(x, held.at[c])
            out(c, x).start()

        def on_whole(g):
            o_ref[:, pl.ds(pl.multiple_of(2 * half + g * WIDE, WIDE), WIDE)] = term(x, full.at[g])

        by_kind(u, on_split, on_whole)

    def turn(i):
        yy, xx = group(i)
        for side in range(2):
            tall = windows[yy, xx, side].T
            at = pl.multiple_of(((yy * 2 + xx) * 2 + side) * LANES, LANES)
            for k in range(2):
                left[k, :, pl.ds(at, LANES)] = tall[k * rows:(k + 1) * rows]

    def send_swap(c, carry):
        for j in range(STRIPS):
            give_in(c, j).wait()
        swap(c).start()
        return carry

    first = min(split, max(places[0], 1))
    send_swap(0, 0)
    a_in(0).wait()
    a_in(1).wait()
    a_out(1).start()
    lax.fori_loop(1, min(2, first), send_swap, 0)
    a_out(0).start()
    over(3, core).start()
    lax.fori_loop(min(2, first), first, send_swap, 0)

    def step(s, carry):
        @pl.when(s < units)
        def _():
            start_own(s)

        for hop in range(depth - 1, 0, -1):
            @pl.when((s >= hop) & (s - hop < units))
            def _():
                pass_on(s - hop, hop)

        @pl.when(s == 1)
        def _():
            a_wait(1)
            a_out(2).start()
            over(1, core).start()
            for g in range(whole):
                for j in range(STRIPS):
                    full_in(g, j).wait()
                full_x(g, x).start()
            lax.fori_loop(first, split, send_swap, 0)

        @pl.when(s == 2)
        def _():
            a_wait(0)
            over(0, core).start()

        @pl.when(s == depth - 1)
        def _():
            for g in range(whole):
                full_x(g, 1 - x).wait_recv()
                full_y(g, y).start()
            for i in (3, 1, 0):
                over(i, 1 - core).wait_recv()
                turn(i)

        @pl.when(s == depth)
        def _():
            a_wait(2)
            over(2, core).start()
            over(2, 1 - core).wait_recv()
            turn(2)

        @pl.when(s >= depth)
        def _():
            multiply(s - depth)

        return carry

    lax.fori_loop(0, units + depth, step, 0)

    for i in range(3):
        a_out(i).wait_send()
    for i in range(4):
        over(i, core).wait_send()
    for g in range(whole):
        full_x(g, x).wait_send()
        full_y(g, y).wait_send()

    def drain(u, carry):
        def lines(ref_of):
            for source in range(depth):
                @pl.when((z < depth - 1) & (z >= source))
                def _():
                    line(u, ref_of(source), source, 1).wait_send()

                @pl.when((z > 0) & (z <= source))
                def _():
                    line(u, ref_of(source), source, 0).wait_send()

        def on_split(c):
            lines(lambda s: held.at[c, y, :, s])
            swap(c).wait_send()
            for source in range(depth):
                to_y(u, c, source, y).wait_send()
            out(c, x).wait_send()
            out(c, 1 - x).wait_recv()

        by_kind(u, on_split, lambda g: lines(lambda s: full.at[g, :, :, s]))
        return carry

    lax.fori_loop(0, units, drain, 0)


def gathered(shape, inputs, out_grad):
    depth = shape["din"]
    groups = shape["tok"]
    rows = inputs.shape[1] // groups
    piece = inputs.shape[0]
    tall, columns = out_grad.shape
    split, whole, places = plan(columns)
    units = split + whole
    tokens = tall * depth * groups
    kind = out_grad.dtype
    dma = pltpu.SemaphoreType.DMA
    return pl.pallas_call(
        functools.partial(kernel, (depth, split, whole, places, rows)),
        out_shape=jax.ShapeDtypeStruct((rows, columns), kind),
        in_specs=[pl.BlockSpec(memory_space=pltpu.HBM)] * 2,
        out_specs=pl.BlockSpec(memory_space=pltpu.VMEM),
        scratch_shapes=[
            pltpu.VMEM((split, STRIPS, tall, LANES), kind),
            pltpu.VMEM((split, 2, 2, depth, STRIPS, tall, LANES), kind),
            pltpu.VMEM((whole, 2, 2, depth, STRIPS, tall, LANES), kind),
            pltpu.VMEM((piece, 2 * rows), kind),
            pltpu.VMEM((2, 2, 2, piece, 2 * rows), kind),
            pltpu.VMEM((2, rows, tokens), kind),
            pltpu.VMEM((split, rows, WIDE), kind),
            dma((split, STRIPS)),
            dma((split, STRIPS)),
            dma((whole, STRIPS)),
            dma((2,)),
            dma((split,)),
            dma((split,)),
            dma((whole,)),
            dma((whole,)),
            dma((whole,)),
            dma((whole,)),
            dma((3,)),
            dma((3,)),
            dma((4,)),
            dma((4,)),
            dma((units, depth, 2)),
            dma((units, depth)),
            dma((units, depth)),
            dma((units, depth)),
            dma((split,)),
            dma((split,)),
        ],
        compiler_params=pltpu.CompilerParams(
            collective_id=0, has_side_effects=True, vmem_limit_bytes=59 * 2**20
        ),
        cost_estimate=pl.CostEstimate(
            flops=2 * rows * tokens * columns,
            bytes_accessed=2 * rows * columns,
            transcendentals=0,
        ),
    )(inputs, out_grad)


def solution(mesh):
    shape = dict(mesh.shape)

    def local(inputs, out_grad):
        groups, depth = shape["tok"], shape["din"]
        rows = inputs.shape[1] // groups
        tall, columns = out_grad.shape
        fits = (
            groups == 4
            and shape["dout"] == 2
            and 2 < depth <= 8
            and inputs.shape[0] == LANES
            and tall * depth == 2 * LANES
            and rows % 64 == 0
            and tall % 16 == 0
            and columns % WIDE == 0
            and columns >= 8 * WIDE
            and rows * columns <= 2**21
        )
        if fits:
            return gathered(shape, inputs, out_grad)
        return scattered(inputs, out_grad)

    placed = (P(("tok", "dout"), "din"), P(("tok", "din"), "dout"))
    return jax.shard_map(
        local, mesh=mesh, in_specs=placed, out_specs=P(("din", "tok"), "dout"), check_vma=False
    )
```

```python
import functools

import jax
import jax.numpy as jnp
from jax import lax
from jax.experimental import pallas as pl
from jax.experimental.pallas import tpu as pltpu
from jax.sharding import PartitionSpec as P

MESH = pl.DeviceIdType.MESH
LANES = 128
STRIPS = 2
WIDE = STRIPS * LANES


def scattered(inputs, out_grad):
    gathered = lax.all_gather(inputs, "dout", axis=0, tiled=True)
    partial_term = lax.dot_general(
        gathered,
        lax.all_gather(out_grad, "din", axis=0, tiled=True),
        (((0,), (0,)), ((), ())),
        preferred_element_type=jnp.float32,
    )
    return lax.psum_scatter(
        partial_term.astype(jnp.bfloat16), "tok", scatter_dimension=0, tiled=True
    )


def plan(columns):
    total = columns // WIDE
    whole = 2 - total % 2
    split = (total - whole) // 2
    places = [(split * (g + 1)) // whole + g if g < whole - 1 else split + g for g in range(whole)]
    return split, whole, places


def kernel(sizes, a_ref, g_ref, o_ref, give, held, full, away, windows, left, ship,
           give_load, own_load, full_load, a_load,
           swap_send, swap_recv, fx_send, fx_recv, fy_send, fy_recv,
           a_send, a_recv, p_send, p_recv,
           z_send, z_recv, y_send, y_recv, out_send, out_recv):
    depth, split, whole, places, rows = sizes
    units = split + whole
    t, z, core = lax.axis_index("tok"), lax.axis_index("din"), lax.axis_index("dout")
    y, x = t // 2, t % 2
    near_x = (y * 2 + (1 - x), z, core)
    near_y = ((1 - y) * 2 + x, z, core)
    partner = (t, z, 1 - core)
    half = split * WIDE
    pair = 2 * rows

    def columns_of(side, c):
        return pl.multiple_of(side * half + c * WIDE, WIDE)

    def strip(start, j):
        return g_ref.at[:, pl.ds(pl.multiple_of(start + j * LANES, LANES), LANES)]

    def give_in(c, j):
        return pltpu.make_async_copy(strip(columns_of(1 - x, c), j), give.at[c, j], give_load.at[c, j])

    def own_in(c, j):
        return pltpu.make_async_copy(strip(columns_of(x, c), j), held.at[c, y, x, z, j], own_load.at[c, j])

    def full_in(g, j):
        return pltpu.make_async_copy(
            strip(2 * half + g * WIDE, j), full.at[g, y, x, z, j], full_load.at[g, j]
        )

    def a_in(i):
        src = a_ref.at[:, pl.ds(pl.multiple_of((y if i == 0 else 1 - y) * pair, LANES), pair)]
        return pltpu.make_async_copy(src, windows.at[y, x, core] if i == 0 else away, a_load.at[i])

    def load(c, carry):
        for j in range(STRIPS):
            give_in(c, j).start()
            own_in(c, j).start()
        return carry

    load(0, 0)
    a_in(0).start()
    a_in(1).start()
    lax.fori_loop(1, split, load, 0)
    for g in range(whole):
        for j in range(STRIPS):
            full_in(g, j).start()

    barrier = pltpu.get_barrier_semaphore()
    for other in (near_x, near_y, partner):
        pl.semaphore_signal(barrier, inc=1, device_id=other, device_id_type=MESH)

    @pl.when(z > 0)
    def _():
        pl.semaphore_signal(barrier, inc=1, device_id=(t, z - 1, core), device_id_type=MESH)

    @pl.when(z < depth - 1)
    def _():
        pl.semaphore_signal(barrier, inc=1, device_id=(t, z + 1, core), device_id_type=MESH)

    pl.semaphore_wait(barrier, 3 + jnp.where(z > 0, 1, 0) + jnp.where(z < depth - 1, 1, 0))

    def remote(src, dst, send, recv, device):
        return pltpu.make_async_remote_copy(
            src_ref=src, dst_ref=dst, send_sem=send, recv_sem=recv,
            device_id=device, device_id_type=MESH,
        )

    def swap(c):
        return remote(give.at[c], held.at[c, y, x, z], swap_send.at[c], swap_recv.at[c], near_x)

    def swap_wait(c):
        ref = held.at[c, y, 1 - x, z]
        remote(ref, ref, swap_send.at[c], swap_recv.at[c], near_x).wait_recv()

    def full_x(g, side):
        ref = full.at[g, y, side, z]
        return remote(ref, ref, fx_send.at[g], fx_recv.at[g], near_x)

    def full_y(g, row):
        ref = full.at[g, row, :, z]
        return remote(ref, ref, fy_send.at[g], fy_recv.at[g], near_y)

    def a_out(i):
        src = (windows.at[y, x, core], away, windows.at[1 - y, x, core])[i]
        dst = (windows.at[y, x, core], windows.at[y, x, core], windows.at[1 - y, x, core])[i]
        return remote(src, dst, a_send.at[i], a_recv.at[i], near_y if i == 1 else near_x)

    def a_wait(i):
        ref = (windows.at[y, 1 - x, core], windows.at[1 - y, x, core], windows.at[1 - y, 1 - x, core])[i]
        remote(ref, ref, a_send.at[i], a_recv.at[i], near_y if i == 1 else near_x).wait_recv()

    def group(i):
        return ((y, 1 - x), (1 - y, x), (1 - y, 1 - x), (y, x))[i]

    def over(i, side):
        yy, xx = group(i)
        ref = windows.at[yy, xx, side]
        return remote(ref, ref, p_send.at[i], p_recv.at[i], partner)

    def line(u, ref, source, up):
        return remote(
            ref, ref, z_send.at[u, source, up], z_recv.at[u, source],
            (t, z + 1 if up else z - 1, core),
        )

    def to_y(u, c, source, row):
        ref = held.at[c, row, :, source]
        return remote(ref, ref, y_send.at[u, source], y_recv.at[u, source], near_y)

    def by_kind(u, on_split, on_whole):
        is_whole = functools.reduce(jnp.logical_or, [u == p for p in places])
        before = sum(jnp.where(u > p, 1, 0) for p in places)

        @pl.when(jnp.logical_not(is_whole))
        def _():
            on_split(u - before)

        @pl.when(is_whole)
        def _():
            on_whole(before)

    def both_ways(u, ref):
        @pl.when(z < depth - 1)
        def _():
            line(u, ref, z, 1).start()

        @pl.when(z > 0)
        def _():
            line(u, ref, z, 0).start()

    def start_own(u):
        def on_split(c):
            for j in range(STRIPS):
                own_in(c, j).wait()
            swap_wait(c)
            both_ways(u, held.at[c, y, :, z])
            to_y(u, c, z, y).start()

        def on_whole(g):
            full_y(g, 1 - y).wait_recv()
            both_ways(u, full.at[g, :, :, z])

        by_kind(u, on_split, on_whole)

    def pass_on(u, hop):
        def on(of, then):
            @pl.when(z - hop >= 0)
            def _():
                ref = of(z - hop)
                line(u, ref, z - hop, 0).wait_recv()

                @pl.when(z < depth - 1)
                def _():
                    line(u, ref, z - hop, 1).start()

                then(z - hop)

            @pl.when(z + hop < depth)
            def _():
                ref = of(z + hop)
                line(u, ref, z + hop, 1).wait_recv()

                @pl.when(z > 0)
                def _():
                    line(u, ref, z + hop, 0).start()

                then(z + hop)

        by_kind(
            u,
            lambda c: on(lambda s: held.at[c, y, :, s], lambda s: to_y(u, c, s, y).start()),
            lambda g: on(lambda s: full.at[g, :, :, s], lambda s: None),
        )

    def out(c, side):
        dst = o_ref.at[:, pl.ds(columns_of(side, c), WIDE)]
        return remote(ship.at[c], dst, out_send.at[c], out_recv.at[c], near_x)

    def term(side, block):
        wide = jnp.concatenate([block[:, :, :, j].reshape(-1, LANES) for j in range(STRIPS)], axis=1)
        return jnp.dot(left[side], wide, preferred_element_type=jnp.float32).astype(o_ref.dtype)

    def multiply(u):
        def on_split(c):
            for source in range(depth):
                to_y(u, c, source, 1 - y).wait_recv()
            ship[c] = term(1 - x, held.at[c])
            o_ref[:, pl.ds(columns_of(x, c), WIDE)] = term(x, held.at[c])
            out(c, x).start()

        def on_whole(g):
            o_ref[:, pl.ds(pl.multiple_of(2 * half + g * WIDE, WIDE), WIDE)] = term(x, full.at[g])

        by_kind(u, on_split, on_whole)

    def turn(i):
        yy, xx = group(i)
        for side in range(2):
            tall = windows[yy, xx, side].T
            at = pl.multiple_of(((yy * 2 + xx) * 2 + side) * LANES, LANES)
            for k in range(2):
                left[k, :, pl.ds(at, LANES)] = tall[k * rows:(k + 1) * rows]

    def send_swap(c, carry):
        for j in range(STRIPS):
            give_in(c, j).wait()
        swap(c).start()
        return carry

    first = min(split, max(places[0], 1))
    send_swap(0, 0)
    a_in(0).wait()
    a_in(1).wait()
    a_out(1).start()
    lax.fori_loop(1, min(2, first), send_swap, 0)
    a_out(0).start()
    over(3, core).start()
    lax.fori_loop(min(2, first), first, send_swap, 0)

    def step(s, carry):
        @pl.when(s < units)
        def _():
            start_own(s)

        for hop in range(depth - 1, 0, -1):
            @pl.when((s >= hop) & (s - hop < units))
            def _():
                pass_on(s - hop, hop)

        @pl.when(s == 1)
        def _():
            a_wait(1)
            a_out(2).start()
            over(1, core).start()
            for g in range(whole):
                for j in range(STRIPS):
                    full_in(g, j).wait()
                full_x(g, x).start()
            lax.fori_loop(first, split, send_swap, 0)

        @pl.when(s == 2)
        def _():
            a_wait(0)
            over(0, core).start()

        @pl.when(s == depth - 1)
        def _():
            for g in range(whole):
                full_x(g, 1 - x).wait_recv()
                full_y(g, y).start()
            for i in (3, 1, 0):
                over(i, 1 - core).wait_recv()
                turn(i)

        @pl.when(s == depth)
        def _():
            a_wait(2)
            over(2, core).start()
            over(2, 1 - core).wait_recv()
            turn(2)

        @pl.when(s >= depth)
        def _():
            multiply(s - depth)

        return carry

    lax.fori_loop(0, units + depth, step, 0)

    for i in range(3):
        a_out(i).wait_send()
    for i in range(4):
        over(i, core).wait_send()
    for g in range(whole):
        full_x(g, x).wait_send()
        full_y(g, y).wait_send()

    def drain(u, carry):
        def lines(ref_of):
            for source in range(depth):
                @pl.when((z < depth - 1) & (z >= source))
                def _():
                    line(u, ref_of(source), source, 1).wait_send()

                @pl.when((z > 0) & (z <= source))
                def _():
                    line(u, ref_of(source), source, 0).wait_send()

        def on_split(c):
            lines(lambda s: held.at[c, y, :, s])
            swap(c).wait_send()
            for source in range(depth):
                to_y(u, c, source, y).wait_send()
            out(c, x).wait_send()
            out(c, 1 - x).wait_recv()

        by_kind(u, on_split, lambda g: lines(lambda s: full.at[g, :, :, s]))
        return carry

    lax.fori_loop(0, units, drain, 0)


def gathered(shape, inputs, out_grad):
    depth = shape["din"]
    groups = shape["tok"]
    rows = inputs.shape[1] // groups
    piece = inputs.shape[0]
    tall, columns = out_grad.shape
    split, whole, places = plan(columns)
    units = split + whole
    tokens = tall * depth * groups
    kind = out_grad.dtype
    dma = pltpu.SemaphoreType.DMA
    return pl.pallas_call(
        functools.partial(kernel, (depth, split, whole, places, rows)),
        out_shape=jax.ShapeDtypeStruct((rows, columns), kind),
        in_specs=[pl.BlockSpec(memory_space=pltpu.HBM)] * 2,
        out_specs=pl.BlockSpec(memory_space=pltpu.VMEM),
        scratch_shapes=[
            pltpu.VMEM((split, STRIPS, tall, LANES), kind),
            pltpu.VMEM((split, 2, 2, depth, STRIPS, tall, LANES), kind),
            pltpu.VMEM((whole, 2, 2, depth, STRIPS, tall, LANES), kind),
            pltpu.VMEM((piece, 2 * rows), kind),
            pltpu.VMEM((2, 2, 2, piece, 2 * rows), kind),
            pltpu.VMEM((2, rows, tokens), kind),
            pltpu.VMEM((split, rows, WIDE), kind),
            dma((split, STRIPS)),
            dma((split, STRIPS)),
            dma((whole, STRIPS)),
            dma((2,)),
            dma((split,)),
            dma((split,)),
            dma((whole,)),
            dma((whole,)),
            dma((whole,)),
            dma((whole,)),
            dma((3,)),
            dma((3,)),
            dma((4,)),
            dma((4,)),
            dma((units, depth, 2)),
            dma((units, depth)),
            dma((units, depth)),
            dma((units, depth)),
            dma((split,)),
            dma((split,)),
        ],
        compiler_params=pltpu.CompilerParams(
            collective_id=0, has_side_effects=True, vmem_limit_bytes=40 * 2**20
        ),
        cost_estimate=pl.CostEstimate(
            flops=2 * rows * tokens * columns,
            bytes_accessed=2 * rows * columns,
            transcendentals=0,
        ),
    )(*[pltpu.with_memory_space_constraint(v, pltpu.HBM) for v in (inputs, out_grad)])


def solution(mesh):
    shape = dict(mesh.shape)

    def local(inputs, out_grad):
        groups, depth = shape["tok"], shape["din"]
        rows = inputs.shape[1] // groups
        tall, columns = out_grad.shape
        fits = (
            groups == 4
            and shape["dout"] == 2
            and 2 < depth <= 8
            and inputs.shape[0] == LANES
            and tall * depth == 2 * LANES
            and rows % 64 == 0
            and tall % 16 == 0
            and columns % WIDE == 0
            and columns >= 8 * WIDE
            and rows * columns <= 2**21
        )
        if fits:
            return gathered(shape, inputs, out_grad)
        return scattered(inputs, out_grad)

    placed = (P(("tok", "dout"), "din"), P(("tok", "din"), "dout"))
    return jax.shard_map(
        local, mesh=mesh, in_specs=placed, out_specs=P(("din", "tok"), "dout"), check_vma=False
    )
```

```python
import functools

import jax
import jax.numpy as jnp
from jax import lax
from jax.experimental import pallas as pl
from jax.experimental.pallas import tpu as pltpu
from jax.sharding import PartitionSpec as P

MESH = pl.DeviceIdType.MESH
LANES = 128
SPLIT, EARLY, WHOLE = range(3)
SWAP, A_NEAR_Y, A_NEAR_X, A_ON, A_TAKE, TURN_MOST, A_LAST, TURN_LAST, TO_Y, OWN, LINE, MULTIPLY = range(12)
UNITS = [(SPLIT, 1), (SPLIT, 2), (SPLIT, 2), (SPLIT, 2), (SPLIT, 2), (WHOLE, 2), (SPLIT, 2), (SPLIT, 2), (SPLIT, 2), (EARLY, 2)]
ORDER = [
    (0, 1), (1,), (0, 7), (0, 9), (0, 3), (2,), (9, 1), (0, 6), (9, 3),
    (10, 1, 3), (10, 1, 1), (10, 1, -3), (3,), (10, 3, 1), (4,), (0, 4), (10, 1, -1), (9, 7),
    (10, 1, 2), (5,), (0, 2), (10, 3, -3), (10, 1, -2), (0, 0), (0, 5), (8, 9), (10, 3, -1),
    (10, 3, 2), (9, 6), (6,), (10, 3, 3), (7,), (0, 8), (11, 1), (10, 3, -2), (10, 7, -1),
    (10, 7, 1), (9, 9), (10, 7, -3), (10, 7, 3), (10, 7, -2), (10, 6, -3), (10, 7, 2), (10, 6, 1), (11, 3),
    (10, 6, -1), (9, 8), (11, 7), (10, 6, 3), (10, 6, -2), (10, 6, 2), (10, 9, 3), (10, 9, 1), (10, 8, 1),
    (10, 8, -1), (10, 9, -1), (10, 8, 3), (11, 6), (10, 8, -3), (9, 2), (10, 8, -2), (10, 8, 2), (8, 5),
    (10, 9, -3), (10, 9, -2), (9, 0), (10, 9, 2), (11, 9), (10, 2, 1), (10, 2, -1), (11, 8), (9, 4),
    (10, 2, -3), (10, 2, 2), (10, 2, -2), (10, 2, 3), (10, 4, 3), (10, 0, 1), (10, 0, 3), (10, 0, -1), (10, 0, -3),
    (10, 0, -2), (10, 0, 2), (10, 4, 1), (10, 4, -1), (10, 4, -3), (9, 5), (11, 2), (10, 4, 2), (11, 0),
    (10, 4, -2), (11, 4), (10, 5, -1), (10, 5, 1), (10, 5, 3), (10, 5, -2), (10, 5, 2), (10, 5, -3), (11, 5),
]


def scattered(inputs, out_grad):
    gathered = lax.all_gather(inputs, "dout", axis=0, tiled=True)
    partial_term = lax.dot_general(
        gathered,
        lax.all_gather(out_grad, "din", axis=0, tiled=True),
        (((0,), (0,)), ((), ())),
        preferred_element_type=jnp.float32,
    )
    return lax.psum_scatter(
        partial_term.astype(jnp.bfloat16), "tok", scatter_dimension=0, tiled=True
    )


def plan(strips, depth):
    if depth == 4 and sum(n * (1 if form == WHOLE else 2) for form, n in UNITS) == strips:
        return UNITS, ORDER
    units = [(SPLIT, 2)] * (strips // 4) + [(WHOLE, 2)] * (strips % 4 // 2)
    return units, plain_order(units, depth)


def plain_order(units, depth):
    reach = depth - 1
    split = [u for u, (kind, _) in enumerate(units) if kind != WHOLE]
    acts = [(SWAP, split[0]), (A_NEAR_Y,)] + [(SWAP, u) for u in split[1:5]] + [(A_NEAR_X,)]
    acts += [(SWAP, u) for u in range(len(units)) if u not in split] + [(SWAP, u) for u in split[5:]]
    for s in range(len(units) + reach):
        if s < len(units):
            acts += [(TO_Y, s)] if units[s][0] != SPLIT else []
            acts.append((OWN, s))
        for hop in range(reach - 1, 0, -1):
            if 0 <= s - hop < len(units):
                acts += [(LINE, s - hop, -hop), (LINE, s - hop, hop)]
                if hop == reach - 1:
                    acts += [(LINE, s - hop, -reach), (LINE, s - hop, reach)]
        if s == 1:
            acts += [(A_ON,)]
        if s == 2:
            acts += [(A_TAKE,), (TURN_MOST,), (A_LAST,), (TURN_LAST,)]
        if s >= reach:
            acts.append((MULTIPLY, s - reach))
    return acts


def kernel(sizes, a_ref, g_ref, o_ref, *scratch):
    depth, rows, units, order = sizes
    count = len(units)
    scratch = list(scratch)
    held = [scratch.pop(0) for _ in units]
    give = [scratch.pop(0) if kind != WHOLE else None for kind, _ in units]
    ship = [scratch.pop(0) if kind != WHOLE else None for kind, _ in units]
    (away, windows, left, own_load, give_load, a_load, a_send, a_recv, p_send, p_recv,
     x_send, x_recv, y_send, y_recv, z_send, z_recv, out_send, out_recv) = scratch
    t, z, core = lax.axis_index("tok"), lax.axis_index("din"), lax.axis_index("dout")
    y, x = t // 2, t % 2
    near_x = (y * 2 + (1 - x), z, core)
    near_y = ((1 - y) * 2 + x, z, core)
    partner = (t, z, 1 - core)
    ends = ((z == 0, depth - 1), (z == depth - 1, 0))
    half = sum(n for kind, n in units if kind != WHOLE) * LANES
    pair = 2 * rows
    starts = []
    for u, (kind, _) in enumerate(units):
        alike = [n for k, n in units[:u] if (k == WHOLE) == (kind == WHOLE)]
        starts.append(sum(alike) * LANES + (2 * half if kind == WHOLE else 0))

    def columns_of(u, side):
        return starts[u] if units[u][0] == WHOLE else pl.multiple_of(side * half + starts[u], LANES)

    def strip(u, side, j):
        return g_ref.at[:, pl.ds(columns_of(u, side) + j * LANES, LANES)]

    def own_in(u, j):
        return pltpu.make_async_copy(strip(u, x, j), held[u].at[y, x, z, j], own_load.at[u, j])

    def give_in(u, j):
        return pltpu.make_async_copy(strip(u, 1 - x, j), give[u].at[j], give_load.at[u, j])

    def a_in(i):
        src = a_ref.at[:, pl.ds(pl.multiple_of((y if i == 0 else 1 - y) * pair, LANES), pair)]
        return pltpu.make_async_copy(src, windows.at[y, x, core] if i == 0 else away, a_load.at[i])

    def load(u):
        for j in range(units[u][1]):
            if units[u][0] != WHOLE:
                give_in(u, j).start()
            own_in(u, j).start()

    first = next(act[1] for act in order if act[0] == SWAP)
    load(first)
    for i in (1, 0):
        a_in(i).start()
    for u in range(count):
        if u != first:
            load(u)

    barrier = pltpu.get_barrier_semaphore()
    for other in (near_x, near_y, partner):
        pl.semaphore_signal(barrier, inc=1, device_id=other, device_id_type=MESH)
    greeted = 3
    for there, to in ((z > 0, z - 1), (z < depth - 1, z + 1)) + ends:
        greeted += jnp.where(there, 1, 0)

        @pl.when(there)
        def _():
            pl.semaphore_signal(barrier, inc=1, device_id=(t, to, core), device_id_type=MESH)

    pl.semaphore_wait(barrier, greeted)

    def remote(src, dst, send, recv, device):
        return pltpu.make_async_remote_copy(
            src_ref=src, dst_ref=dst, send_sem=send, recv_sem=recv,
            device_id=device, device_id_type=MESH,
        )

    def swap(u):
        dst = held[u].at[y, x, z]
        return remote(dst if give[u] is None else give[u], dst, x_send.at[u], x_recv.at[u], near_x)

    def swap_wait(u):
        for j in range(units[u][1]):
            own_in(u, j).wait()
        ref = held[u].at[y, 1 - x, z]
        remote(ref, ref, x_send.at[u], x_recv.at[u], near_x).wait_recv()

    def to_y(u, source, row):
        ref = held[u].at[row, :, source]
        return remote(ref, ref, y_send.at[u, source], y_recv.at[u, source], near_y)

    def a_out(i):
        src = (windows.at[y, x, core], away, windows.at[1 - y, x, core])[i]
        dst = (windows.at[y, x, core], windows.at[y, x, core], windows.at[1 - y, x, core])[i]
        return remote(src, dst, a_send.at[i], a_recv.at[i], near_y if i == 1 else near_x)

    def group(i):
        return ((y, 1 - x), (1 - y, x), (1 - y, 1 - x), (y, x))[i]

    def a_wait(i):
        ref = windows.at[group(i) + (core,)]
        remote(ref, ref, a_send.at[i], a_recv.at[i], near_y if i == 1 else near_x).wait_recv()

    def over(i, side):
        ref = windows.at[group(i) + (side,)]
        return remote(ref, ref, p_send.at[i], p_recv.at[i], partner)

    def turn(i):
        yy, xx = group(i)
        for side in range(2):
            tall = windows[yy, xx, side].T
            at = pl.multiple_of(((yy * 2 + xx) * 2 + side) * LANES, LANES)
            for k in range(2):
                left[k, :, pl.ds(at, LANES)] = tall[k * rows:(k + 1) * rows]

    def line_ref(u, source):
        return held[u].at[y, :, source] if units[u][0] == SPLIT else held[u].at[:, :, source]

    def line(u, source, way, to):
        ref = line_ref(u, source)
        return remote(ref, ref, z_send.at[u, source, way], z_recv.at[u, source], (t, to, core))

    def own_lines(u, act):
        for way, (there, to) in enumerate(((z > 0, z - 1), (z < depth - 1, z + 1)) + ends):
            @pl.when(there)
            def _():
                act(line(u, z, min(way, 2), to))

    def forward(u, off, act):
        if abs(off) + 2 < depth:
            @pl.when((z > 0) if off > 0 else (z < depth - 1))
            def _():
                act(line(u, z + off, int(off < 0), z - 1 if off > 0 else z + 1))

    def there(off):
        return (z + off >= 0) & (z + off < depth)

    def line_step(u, off):
        @pl.when(there(off))
        def _():
            line(u, z + off, 2, z).wait_recv()
            forward(u, off, lambda c: c.start())
            if units[u][0] == SPLIT:
                to_y(u, z + off, y).start()

    def own_step(u):
        if units[u][0] == SPLIT:
            swap_wait(u)
            own_lines(u, lambda c: c.start())
            to_y(u, z, y).start()
        else:
            to_y(u, z, 1 - y).wait_recv()
            own_lines(u, lambda c: c.start())

    def out(u, side):
        dst = o_ref.at[:, pl.ds(columns_of(u, side), units[u][1] * LANES)]
        return remote(ship[u], dst, out_send.at[u], out_recv.at[u], near_x)

    def term(u, side):
        block = [held[u][:, :, :, j].reshape(-1, LANES) for j in range(units[u][1])]
        wide = block[0] if len(block) == 1 else jnp.concatenate(block, axis=1)
        return jnp.dot(left[side], wide, preferred_element_type=jnp.float32).astype(o_ref.dtype)

    def multiply(u):
        kind, n = units[u]
        if kind == SPLIT:
            for source in range(depth):
                to_y(u, source, 1 - y).wait_recv()
        if kind != WHOLE:
            ship[u][...] = term(u, 1 - x)
        o_ref[:, pl.ds(columns_of(u, x), n * LANES)] = term(u, x)
        if kind != WHOLE:
            out(u, x).start()

    for act in order:
        what, rest = act[0], act[1:]
        if what == SWAP:
            u = rest[0]
            for j in range(units[u][1]):
                (own_in if give[u] is None else give_in)(u, j).wait()
            swap(u).start()
        elif what == A_NEAR_Y:
            a_in(1).wait()
            a_out(1).start()
        elif what == A_NEAR_X:
            a_in(0).wait()
            a_out(0).start()
            over(3, core).start()
        elif what == A_ON:
            a_wait(1)
            a_out(2).start()
            over(1, core).start()
        elif what == A_TAKE:
            a_wait(0)
            over(0, core).start()
        elif what == TURN_MOST:
            for i in (3, 1, 0):
                over(i, 1 - core).wait_recv()
                turn(i)
        elif what == A_LAST:
            a_wait(2)
            over(2, core).start()
        elif what == TURN_LAST:
            over(2, 1 - core).wait_recv()
            turn(2)
        elif what == TO_Y:
            u = rest[0]
            if give[u] is None:
                ref = held[u].at[y, 1 - x, z]
                remote(ref, ref, x_send.at[u], x_recv.at[u], near_x).wait_recv()
            else:
                swap_wait(u)
            to_y(u, z, y).start()
        elif what == OWN:
            own_step(*rest)
        elif what == LINE:
            line_step(*rest)
        elif what == MULTIPLY:
            multiply(*rest)

    for i in range(3):
        a_out(i).wait_send()
    for i in range(4):
        over(i, core).wait_send()
    for u, (kind, _) in enumerate(units):
        swap(u).wait_send()
        own_lines(u, lambda c: c.wait_send())
        to_y(u, z, y).wait_send()
        for off in range(1 - depth, depth):
            if off:
                @pl.when(there(off))
                def _():
                    forward(u, off, lambda c: c.wait_send())
                    if kind == SPLIT:
                        to_y(u, z + off, y).wait_send()
        if kind != WHOLE:
            out(u, x).wait_send()
            out(u, 1 - x).wait_recv()


def gathered(shape, inputs, out_grad):
    depth = shape["din"]
    groups = shape["tok"]
    rows = inputs.shape[1] // groups
    piece = inputs.shape[0]
    tall, columns = out_grad.shape
    units, order = plan(columns // LANES, depth)
    count = len(units)
    most = max(n for _, n in units)
    tokens = tall * depth * groups
    kind = out_grad.dtype
    dma = pltpu.SemaphoreType.DMA
    return pl.pallas_call(
        functools.partial(kernel, (depth, rows, units, order)),
        out_shape=jax.ShapeDtypeStruct((rows, columns), kind),
        in_specs=[pl.BlockSpec(memory_space=pltpu.HBM)] * 2,
        out_specs=pl.BlockSpec(memory_space=pltpu.VMEM),
        scratch_shapes=[
            *[pltpu.VMEM((2, 2, depth, n, tall, LANES), kind) for _, n in units],
            *[pltpu.VMEM((n, tall, LANES), kind) for form, n in units if form != WHOLE],
            *[pltpu.VMEM((rows, n * LANES), kind) for form, n in units if form != WHOLE],
            pltpu.VMEM((piece, 2 * rows), kind),
            pltpu.VMEM((2, 2, 2, piece, 2 * rows), kind),
            pltpu.VMEM((2, rows, tokens), kind),
            dma((count, most)),
            dma((count, most)),
            dma((2,)),
            dma((3,)),
            dma((3,)),
            dma((4,)),
            dma((4,)),
            dma((count,)),
            dma((count,)),
            dma((count, depth)),
            dma((count, depth)),
            dma((count, depth, 3)),
            dma((count, depth)),
            dma((count,)),
            dma((count,)),
        ],
        compiler_params=pltpu.CompilerParams(
            collective_id=0, has_side_effects=True, vmem_limit_bytes=40 * 2**20
        ),
        cost_estimate=pl.CostEstimate(
            flops=2 * rows * tokens * columns,
            bytes_accessed=2 * rows * columns,
            transcendentals=0,
        ),
    )(*[pltpu.with_memory_space_constraint(v, pltpu.HBM) for v in (inputs, out_grad)])


def solution(mesh):
    shape = dict(mesh.shape)

    def local(inputs, out_grad):
        groups, depth = shape["tok"], shape["din"]
        rows = inputs.shape[1] // groups
        tall, columns = out_grad.shape
        fits = (
            groups == 4
            and shape["dout"] == 2
            and 2 < depth <= 8
            and inputs.shape[0] == LANES
            and tall * depth == 2 * LANES
            and rows % 64 == 0
            and tall % 16 == 0
            and columns % (2 * LANES) == 0
            and columns >= 16 * LANES
            and rows * columns <= 2**21
        )
        if fits:
            return gathered(shape, inputs, out_grad)
        return scattered(inputs, out_grad)

    placed = (P(("tok", "dout"), "din"), P(("tok", "din"), "dout"))
    return jax.shard_map(
        local, mesh=mesh, in_specs=placed, out_specs=P(("din", "tok"), "dout"), check_vma=False
    )
```

```python
import functools

import jax
import jax.numpy as jnp
from jax import lax
from jax.experimental import pallas as pl
from jax.experimental.pallas import tpu as pltpu
from jax.sharding import PartitionSpec as P

MESH = pl.DeviceIdType.MESH
LANES = 128
SPLIT, SPLIT_EARLY, WHOLE, WHOLE_EARLY = range(4)
SWAP, A_NEAR_Y, A_NEAR_X, A_ON, A_TAKE, TURN_MOST, A_LAST, TURN_LAST, TO_Y, OWN, LINE, MULTIPLY = range(12)
UNITS = [(SPLIT, 1), (SPLIT, 1), (SPLIT, 2), (SPLIT, 2), (SPLIT, 2), (WHOLE, 2), (SPLIT, 2), (WHOLE_EARLY, 2), (SPLIT, 2), (SPLIT_EARLY, 2), (SPLIT, 2)]
ORDER = [
    (0, 8), (0, 0), (0, 1), (0, 10), (1,), (0, 9), (2,), (9, 8), (9, 0),
    (9, 1), (9, 10), (0, 4), (8, 9), (10, 8, 1), (3,), (0, 5), (10, 8, -1), (4,),
    (10, 8, 3), (10, 8, -3), (0, 7), (0, 2), (10, 8, 2), (0, 3), (10, 8, -2), (10, 10, -1), (10, 10, 1),
    (9, 4), (6,), (5,), (9, 9), (0, 6), (10, 10, 2), (10, 10, -2), (10, 10, 3), (10, 0, 1),
    (7,), (11, 8), (10, 10, -3), (10, 1, -1), (10, 1, 1), (10, 1, -3), (10, 0, -1), (9, 6), (11, 10),
    (10, 1, -2), (10, 1, 2), (10, 4, -1), (10, 1, 3), (10, 4, 3), (10, 0, -2), (10, 9, -1), (10, 0, -3), (10, 0, 3),
    (10, 0, 2), (10, 4, 1), (10, 9, 1), (11, 1), (10, 4, 2), (10, 6, 1), (10, 4, -3), (10, 4, -2), (10, 9, -3),
    (11, 0), (8, 7), (9, 2), (10, 9, 2), (10, 9, 3), (10, 6, -1), (10, 9, -2), (9, 3), (11, 9),
    (10, 6, 3), (11, 4), (10, 6, 2), (10, 6, -3), (10, 2, -1), (10, 6, -2), (10, 2, 1), (9, 5), (10, 2, -3),
    (10, 2, -2), (10, 3, -3), (10, 2, 3), (10, 2, 2), (10, 3, 1), (10, 3, -1), (11, 6), (9, 7), (10, 3, -2),
    (10, 3, 3), (10, 5, -3), (10, 3, 2), (11, 2), (10, 5, -1), (11, 3), (10, 7, -1), (10, 5, 1), (10, 7, 1),
    (10, 5, -2), (10, 7, -3), (10, 7, -2), (10, 7, 3), (10, 5, 3), (10, 5, 2), (10, 7, 2), (11, 7), (11, 5),
]


def scattered(inputs, out_grad):
    gathered = lax.all_gather(inputs, "dout", axis=0, tiled=True)
    partial_term = lax.dot_general(
        gathered,
        lax.all_gather(out_grad, "din", axis=0, tiled=True),
        (((0,), (0,)), ((), ())),
        preferred_element_type=jnp.float32,
    )
    return lax.psum_scatter(
        partial_term.astype(jnp.bfloat16), "tok", scatter_dimension=0, tiled=True
    )


def plan(strips, depth):
    if depth == 4 and sum(n * (1 if is_whole(form) else 2) for form, n in UNITS) == strips:
        return UNITS, ORDER
    units = [(SPLIT, 2)] * (strips // 4) + [(WHOLE, 2)] * (strips % 4 // 2)
    return units, plain_order(units, depth)


def is_whole(form):
    return form >= WHOLE


def is_early(form):
    return form % 2 == 1


def plain_order(units, depth):
    reach = depth - 1
    split = [u for u, (form, _) in enumerate(units) if not is_whole(form)]
    acts = [(SWAP, split[0]), (A_NEAR_Y,)] + [(SWAP, u) for u in split[1:5]] + [(A_NEAR_X,)]
    acts += [(SWAP, u) for u in range(len(units)) if u not in split] + [(SWAP, u) for u in split[5:]]
    for s in range(len(units) + reach):
        if s < len(units):
            acts += [(TO_Y, s)] if is_early(units[s][0]) else []
            acts.append((OWN, s))
        for hop in range(reach - 1, 0, -1):
            if 0 <= s - hop < len(units):
                acts += [(LINE, s - hop, -hop), (LINE, s - hop, hop)]
                if hop == reach - 1:
                    acts += [(LINE, s - hop, -reach), (LINE, s - hop, reach)]
        if s == 1:
            acts += [(A_ON,)]
        if s == 2:
            acts += [(A_TAKE,), (TURN_MOST,), (A_LAST,), (TURN_LAST,)]
        if s >= reach:
            acts.append((MULTIPLY, s - reach))
    return acts


def kernel(sizes, a_ref, g_ref, o_ref, *scratch):
    depth, rows, units, order = sizes
    count = len(units)
    scratch = list(scratch)
    held = [scratch.pop(0) for _ in units]
    give = [None if is_whole(form) else scratch.pop(0) for form, _ in units]
    ship = [None if is_whole(form) else scratch.pop(0) for form, _ in units]
    (away, windows, left, own_load, give_load, a_load, a_send, a_recv, p_send, p_recv,
     x_send, x_recv, y_send, y_recv, z_send, z_recv, out_send, out_recv) = scratch
    t, z, core = lax.axis_index("tok"), lax.axis_index("din"), lax.axis_index("dout")
    y, x = t // 2, t % 2
    near_x = (y * 2 + (1 - x), z, core)
    near_y = ((1 - y) * 2 + x, z, core)
    partner = (t, z, 1 - core)
    ends = ((z == 0, depth - 1), (z == depth - 1, 0))
    half = sum(n for form, n in units if not is_whole(form)) * LANES
    pair = 2 * rows
    starts = []
    for u, (form, _) in enumerate(units):
        alike = [n for other, n in units[:u] if is_whole(other) == is_whole(form)]
        starts.append(sum(alike) * LANES + (2 * half if is_whole(form) else 0))

    def columns_of(u, side):
        return starts[u] if is_whole(units[u][0]) else pl.multiple_of(side * half + starts[u], LANES)

    def strip(u, side, j):
        return g_ref.at[:, pl.ds(columns_of(u, side) + j * LANES, LANES)]

    def own_in(u, j):
        return pltpu.make_async_copy(strip(u, x, j), held[u].at[y, x, z, j], own_load.at[u, j])

    def give_in(u, j):
        return pltpu.make_async_copy(strip(u, 1 - x, j), give[u].at[j], give_load.at[u, j])

    def a_in(i):
        src = a_ref.at[:, pl.ds(pl.multiple_of((y if i == 0 else 1 - y) * pair, LANES), pair)]
        return pltpu.make_async_copy(src, windows.at[y, x, core] if i == 0 else away, a_load.at[i])

    def load(u):
        for j in range(units[u][1]):
            if give[u] is not None:
                give_in(u, j).start()
            own_in(u, j).start()

    first = next(act[1] for act in order if act[0] == SWAP)
    load(first)
    for i in (1, 0):
        a_in(i).start()
    for u in range(count):
        if u != first:
            load(u)

    barrier = pltpu.get_barrier_semaphore()
    for other in (near_x, near_y, partner):
        pl.semaphore_signal(barrier, inc=1, device_id=other, device_id_type=MESH)
    greeted = 3
    for there, to in ((z > 0, z - 1), (z < depth - 1, z + 1)) + ends:
        greeted += jnp.where(there, 1, 0)

        @pl.when(there)
        def _():
            pl.semaphore_signal(barrier, inc=1, device_id=(t, to, core), device_id_type=MESH)

    pl.semaphore_wait(barrier, greeted)

    def remote(src, dst, send, recv, device):
        return pltpu.make_async_remote_copy(
            src_ref=src, dst_ref=dst, send_sem=send, recv_sem=recv,
            device_id=device, device_id_type=MESH,
        )

    def swap(u):
        dst = held[u].at[y, x, z]
        return remote(dst if give[u] is None else give[u], dst, x_send.at[u], x_recv.at[u], near_x)

    def swap_wait(u):
        if give[u] is not None:
            for j in range(units[u][1]):
                own_in(u, j).wait()
        ref = held[u].at[y, 1 - x, z]
        remote(ref, ref, x_send.at[u], x_recv.at[u], near_x).wait_recv()

    def to_y(u, source, row):
        ref = held[u].at[row, :, source]
        return remote(ref, ref, y_send.at[u, source], y_recv.at[u, source], near_y)

    def a_out(i):
        src = (windows.at[y, x, core], away, windows.at[1 - y, x, core])[i]
        dst = (windows.at[y, x, core], windows.at[y, x, core], windows.at[1 - y, x, core])[i]
        return remote(src, dst, a_send.at[i], a_recv.at[i], near_y if i == 1 else near_x)

    def group(i):
        return ((y, 1 - x), (1 - y, x), (1 - y, 1 - x), (y, x))[i]

    def a_wait(i):
        ref = windows.at[group(i) + (core,)]
        remote(ref, ref, a_send.at[i], a_recv.at[i], near_y if i == 1 else near_x).wait_recv()

    def over(i, side):
        ref = windows.at[group(i) + (side,)]
        return remote(ref, ref, p_send.at[i], p_recv.at[i], partner)

    def turn(i):
        yy, xx = group(i)
        for side in range(2):
            tall = windows[yy, xx, side].T
            at = pl.multiple_of(((yy * 2 + xx) * 2 + side) * LANES, LANES)
            for k in range(2):
                left[k, :, pl.ds(at, LANES)] = tall[k * rows:(k + 1) * rows]

    def line_ref(u, source):
        return held[u].at[:, :, source] if is_early(units[u][0]) else held[u].at[y, :, source]

    def line(u, source, way, to):
        ref = line_ref(u, source)
        return remote(ref, ref, z_send.at[u, source, way], z_recv.at[u, source], (t, to, core))

    def own_lines(u, act):
        for way, (there, to) in enumerate(((z > 0, z - 1), (z < depth - 1, z + 1)) + ends):
            @pl.when(there)
            def _():
                act(line(u, z, min(way, 2), to))

    def forward(u, off, act):
        if abs(off) + 2 < depth:
            @pl.when((z > 0) if off > 0 else (z < depth - 1))
            def _():
                act(line(u, z + off, int(off < 0), z - 1 if off > 0 else z + 1))

    def there(off):
        return (z + off >= 0) & (z + off < depth)

    def line_step(u, off):
        @pl.when(there(off))
        def _():
            line(u, z + off, 2, z).wait_recv()
            forward(u, off, lambda c: c.start())
            if not is_early(units[u][0]):
                to_y(u, z + off, y).start()

    def own_step(u):
        if is_early(units[u][0]):
            to_y(u, z, 1 - y).wait_recv()
            own_lines(u, lambda c: c.start())
        else:
            swap_wait(u)
            own_lines(u, lambda c: c.start())
            to_y(u, z, y).start()

    def out(u, side):
        dst = o_ref.at[:, pl.ds(columns_of(u, side), units[u][1] * LANES)]
        return remote(ship[u], dst, out_send.at[u], out_recv.at[u], near_x)

    def term(u, side):
        block = [held[u][:, :, :, j].reshape(-1, LANES) for j in range(units[u][1])]
        wide = block[0] if len(block) == 1 else jnp.concatenate(block, axis=1)
        return jnp.dot(left[side], wide, preferred_element_type=jnp.float32).astype(o_ref.dtype)

    def multiply(u):
        form, n = units[u]
        if not is_early(form):
            for source in range(depth):
                to_y(u, source, 1 - y).wait_recv()
        if not is_whole(form):
            ship[u][...] = term(u, 1 - x)
        o_ref[:, pl.ds(columns_of(u, x), n * LANES)] = term(u, x)
        if not is_whole(form):
            out(u, x).start()

    for act in order:
        what, rest = act[0], act[1:]
        if what == SWAP:
            u = rest[0]
            for j in range(units[u][1]):
                (own_in if give[u] is None else give_in)(u, j).wait()
            swap(u).start()
        elif what == A_NEAR_Y:
            a_in(1).wait()
            a_out(1).start()
        elif what == A_NEAR_X:
            a_in(0).wait()
            a_out(0).start()
            over(3, core).start()
        elif what == A_ON:
            a_wait(1)
            a_out(2).start()
            over(1, core).start()
        elif what == A_TAKE:
            a_wait(0)
            over(0, core).start()
        elif what == TURN_MOST:
            for i in (3, 1, 0):
                over(i, 1 - core).wait_recv()
                turn(i)
        elif what == A_LAST:
            a_wait(2)
            over(2, core).start()
        elif what == TURN_LAST:
            over(2, 1 - core).wait_recv()
            turn(2)
        elif what == TO_Y:
            u = rest[0]
            swap_wait(u)
            to_y(u, z, y).start()
        elif what == OWN:
            own_step(*rest)
        elif what == LINE:
            line_step(*rest)
        elif what == MULTIPLY:
            multiply(*rest)

    for i in range(3):
        a_out(i).wait_send()
    for i in range(4):
        over(i, core).wait_send()
    for u, (form, _) in enumerate(units):
        swap(u).wait_send()
        own_lines(u, lambda c: c.wait_send())
        to_y(u, z, y).wait_send()
        for off in range(1 - depth, depth):
            if off:
                @pl.when(there(off))
                def _():
                    forward(u, off, lambda c: c.wait_send())
                    if not is_early(form):
                        to_y(u, z + off, y).wait_send()
        if not is_whole(form):
            out(u, x).wait_send()
            out(u, 1 - x).wait_recv()


def gathered(shape, inputs, out_grad):
    depth = shape["din"]
    groups = shape["tok"]
    rows = inputs.shape[1] // groups
    piece = inputs.shape[0]
    tall, columns = out_grad.shape
    units, order = plan(columns // LANES, depth)
    count = len(units)
    most = max(n for _, n in units)
    tokens = tall * depth * groups
    kind = out_grad.dtype
    dma = pltpu.SemaphoreType.DMA
    return pl.pallas_call(
        functools.partial(kernel, (depth, rows, units, order)),
        out_shape=jax.ShapeDtypeStruct((rows, columns), kind),
        in_specs=[pl.BlockSpec(memory_space=pltpu.HBM)] * 2,
        out_specs=pl.BlockSpec(memory_space=pltpu.VMEM),
        scratch_shapes=[
            *[pltpu.VMEM((2, 2, depth, n, tall, LANES), kind) for _, n in units],
            *[pltpu.VMEM((n, tall, LANES), kind) for form, n in units if not is_whole(form)],
            *[pltpu.VMEM((rows, n * LANES), kind) for form, n in units if not is_whole(form)],
            pltpu.VMEM((piece, 2 * rows), kind),
            pltpu.VMEM((2, 2, 2, piece, 2 * rows), kind),
            pltpu.VMEM((2, rows, tokens), kind),
            dma((count, most)),
            dma((count, most)),
            dma((2,)),
            dma((3,)),
            dma((3,)),
            dma((4,)),
            dma((4,)),
            dma((count,)),
            dma((count,)),
            dma((count, depth)),
            dma((count, depth)),
            dma((count, depth, 3)),
            dma((count, depth)),
            dma((count,)),
            dma((count,)),
        ],
        compiler_params=pltpu.CompilerParams(
            collective_id=0, has_side_effects=True, vmem_limit_bytes=40 * 2**20
        ),
        cost_estimate=pl.CostEstimate(
            flops=2 * rows * tokens * columns,
            bytes_accessed=2 * rows * columns,
            transcendentals=0,
        ),
    )(*[pltpu.with_memory_space_constraint(v, pltpu.HBM) for v in (inputs, out_grad)])


def solution(mesh):
    shape = dict(mesh.shape)

    def local(inputs, out_grad):
        groups, depth = shape["tok"], shape["din"]
        rows = inputs.shape[1] // groups
        tall, columns = out_grad.shape
        fits = (
            groups == 4
            and shape["dout"] == 2
            and 2 < depth <= 8
            and inputs.shape[0] == LANES
            and tall * depth == 2 * LANES
            and rows % 64 == 0
            and tall % 16 == 0
            and columns % (2 * LANES) == 0
            and columns >= 16 * LANES
            and rows * columns <= 2**21
        )
        if fits:
            return gathered(shape, inputs, out_grad)
        return scattered(inputs, out_grad)

    placed = (P(("tok", "dout"), "din"), P(("tok", "din"), "dout"))
    return jax.shard_map(
        local, mesh=mesh, in_specs=placed, out_specs=P(("din", "tok"), "dout"), check_vma=False
    )
```

```python
import functools

import jax
import jax.numpy as jnp
from jax import lax
from jax.experimental import pallas as pl
from jax.experimental.pallas import tpu as pltpu
from jax.sharding import PartitionSpec as P

MESH = pl.DeviceIdType.MESH
LANES = 128
SPLIT, SPLIT_EARLY, WHOLE, WHOLE_EARLY = range(4)
SWAP, A_NEAR_Y, A_NEAR_X, A_ON, A_TAKE, TURN_MOST, A_LAST, TURN_LAST, TO_Y, OWN, LINE, MULTIPLY, A_OTHER_X = range(13)
UNITS = [(SPLIT, 1), (SPLIT, 1), (SPLIT, 2), (SPLIT, 2), (SPLIT, 2), (WHOLE, 2), (SPLIT, 2), (WHOLE_EARLY, 2), (SPLIT, 2), (SPLIT_EARLY, 2), (SPLIT, 2)]
ORDER = [
    (1,), (0, 8), (0, 10), (0, 9), (0, 6), (2,), (12,), (9, 8), (9, 10),
    (10, 8, -1), (0, 4), (10, 8, 1), (9, 6), (3,), (8, 9), (10, 8, -2), (10, 8, 3), (0, 0),
    (10, 8, -3), (4,), (10, 8, 2), (10, 10, -1), (10, 10, 1), (5,), (9, 4), (0, 7), (0, 5),
    (6,), (0, 1), (10, 10, 3), (0, 2), (10, 10, -3), (10, 10, 2), (10, 10, -2), (10, 6, 1), (0, 3),
    (10, 6, -1), (9, 0), (10, 6, 3), (7,), (9, 9), (11, 8), (10, 6, -2), (10, 6, -3), (11, 10),
    (10, 6, 2), (10, 0, 1), (10, 0, -1), (10, 0, 3), (10, 4, -1), (10, 4, 1), (10, 9, 1), (10, 0, -3), (10, 0, -2),
    (10, 0, 2), (10, 9, -1), (10, 4, -3), (9, 2), (11, 6), (10, 4, -2), (10, 4, 2), (10, 4, 3), (8, 7),
    (11, 0), (10, 9, 3), (9, 3), (11, 4), (10, 9, 2), (10, 2, 1), (10, 2, -3), (10, 2, -1), (10, 2, 3),
    (10, 9, -3), (9, 1), (10, 3, 3), (10, 9, -2), (11, 9), (10, 3, -1), (10, 2, -2), (10, 2, 2), (10, 3, -3),
    (10, 3, 1), (9, 5), (10, 1, -1), (10, 3, -2), (11, 2), (10, 3, 2), (10, 1, 1), (10, 1, -3), (10, 1, -2),
    (9, 7), (10, 5, -1), (10, 5, 1), (10, 1, 3), (10, 5, 3), (10, 1, 2), (11, 3), (10, 7, 1), (10, 5, -3),
    (10, 5, -2), (10, 5, 2), (10, 7, -1), (11, 1), (11, 5), (10, 7, -2), (10, 7, 2), (10, 7, 3), (10, 7, -3),
    (11, 7),
]


def scattered(inputs, out_grad):
    gathered = lax.all_gather(inputs, "dout", axis=0, tiled=True)
    partial_term = lax.dot_general(
        gathered,
        lax.all_gather(out_grad, "din", axis=0, tiled=True),
        (((0,), (0,)), ((), ())),
        preferred_element_type=jnp.float32,
    )
    return lax.psum_scatter(
        partial_term.astype(jnp.bfloat16), "tok", scatter_dimension=0, tiled=True
    )


def plan(strips, depth):
    if depth == 4 and sum(n * (1 if is_whole(form) else 2) for form, n in UNITS) == strips:
        return UNITS, ORDER
    units = [(SPLIT, 2)] * (strips // 4) + [(WHOLE, 2)] * (strips % 4 // 2)
    return units, plain_order(units, depth)


def is_whole(form):
    return form >= WHOLE


def is_early(form):
    return form % 2 == 1


def plain_order(units, depth):
    reach = depth - 1
    split = [u for u, (form, _) in enumerate(units) if not is_whole(form)]
    acts = [(SWAP, split[0]), (A_NEAR_Y,)] + [(SWAP, u) for u in split[1:5]] + [(A_NEAR_X,), (A_OTHER_X,)]
    acts += [(SWAP, u) for u in range(len(units)) if u not in split] + [(SWAP, u) for u in split[5:]]
    for s in range(len(units) + reach):
        if s < len(units):
            acts += [(TO_Y, s)] if is_early(units[s][0]) else []
            acts.append((OWN, s))
        for hop in range(reach - 1, 0, -1):
            if 0 <= s - hop < len(units):
                acts += [(LINE, s - hop, -hop), (LINE, s - hop, hop)]
                if hop == reach - 1:
                    acts += [(LINE, s - hop, -reach), (LINE, s - hop, reach)]
        if s == 1:
            acts += [(A_ON,)]
        if s == 2:
            acts += [(A_TAKE,), (TURN_MOST,), (A_LAST,), (TURN_LAST,)]
        if s >= reach:
            acts.append((MULTIPLY, s - reach))
    return acts


def kernel(sizes, a_ref, g_ref, o_ref, *scratch):
    depth, rows, units, order = sizes
    count = len(units)
    scratch = list(scratch)
    held = [scratch.pop(0) for _ in units]
    give = [None if is_whole(form) else scratch.pop(0) for form, _ in units]
    ship = [None if is_whole(form) else scratch.pop(0) for form, _ in units]
    (away, windows, left, own_load, give_load, a_load, a_send, a_recv, p_send, p_recv,
     x_send, x_recv, y_send, y_recv, z_send, z_recv, out_send, out_recv) = scratch
    t, z, core = lax.axis_index("tok"), lax.axis_index("din"), lax.axis_index("dout")
    y, x = t // 2, t % 2
    near_x = (y * 2 + (1 - x), z, core)
    near_y = ((1 - y) * 2 + x, z, core)
    partner = (t, z, 1 - core)
    ends = ((z == 0, depth - 1), (z == depth - 1, 0))
    half = sum(n for form, n in units if not is_whole(form)) * LANES
    pair = 2 * rows
    starts = []
    for u, (form, _) in enumerate(units):
        alike = [n for other, n in units[:u] if is_whole(other) == is_whole(form)]
        starts.append(sum(alike) * LANES + (2 * half if is_whole(form) else 0))

    def columns_of(u, side):
        return starts[u] if is_whole(units[u][0]) else pl.multiple_of(side * half + starts[u], LANES)

    def strip(u, side, j):
        return g_ref.at[:, pl.ds(columns_of(u, side) + j * LANES, LANES)]

    def own_in(u, j):
        return pltpu.make_async_copy(strip(u, x, j), held[u].at[y, x, z, j], own_load.at[u, j])

    def give_in(u, j):
        return pltpu.make_async_copy(strip(u, 1 - x, j), give[u].at[j], give_load.at[u, j])

    def a_in(i):
        src = a_ref.at[:, pl.ds(pl.multiple_of((y if i == 0 else 1 - y) * pair, LANES), pair)]
        return pltpu.make_async_copy(src, windows.at[y, x, core] if i == 0 else away, a_load.at[i])

    def load(u):
        for j in range(units[u][1]):
            if give[u] is not None:
                give_in(u, j).start()
            own_in(u, j).start()

    first = next(act[1] for act in order if act[0] == SWAP)
    load(first)
    for i in (1, 0):
        a_in(i).start()
    for u in range(count):
        if u != first:
            load(u)

    barrier = pltpu.get_barrier_semaphore()
    for other in (near_x, near_y, partner):
        pl.semaphore_signal(barrier, inc=1, device_id=other, device_id_type=MESH)
    greeted = 3
    for there, to in ((z > 0, z - 1), (z < depth - 1, z + 1)) + ends:
        greeted += jnp.where(there, 1, 0)

        @pl.when(there)
        def _():
            pl.semaphore_signal(barrier, inc=1, device_id=(t, to, core), device_id_type=MESH)

    pl.semaphore_wait(barrier, greeted)

    def remote(src, dst, send, recv, device):
        return pltpu.make_async_remote_copy(
            src_ref=src, dst_ref=dst, send_sem=send, recv_sem=recv,
            device_id=device, device_id_type=MESH,
        )

    def swap(u):
        dst = held[u].at[y, x, z]
        return remote(dst if give[u] is None else give[u], dst, x_send.at[u], x_recv.at[u], near_x)

    def swap_wait(u):
        if give[u] is not None:
            for j in range(units[u][1]):
                own_in(u, j).wait()
        ref = held[u].at[y, 1 - x, z]
        remote(ref, ref, x_send.at[u], x_recv.at[u], near_x).wait_recv()

    def to_y(u, source, row):
        ref = held[u].at[row, :, source]
        return remote(ref, ref, y_send.at[u, source], y_recv.at[u, source], near_y)

    def a_out(i):
        src = (windows.at[y, x, core], away, windows.at[1 - y, x, core], windows.at[y, x, 1 - core])[i]
        dst = windows.at[y, x, core] if i == 1 else src
        return remote(src, dst, a_send.at[i], a_recv.at[i], near_y if i == 1 else near_x)

    def group(i):
        return ((y, 1 - x), (1 - y, x), (1 - y, 1 - x), (y, x), (y, 1 - x))[i]

    def a_wait(i):
        yy, xx = group(i) if i < 3 else (y, 1 - x)
        ref = windows.at[yy, xx, 1 - core if i == 3 else core]
        remote(ref, ref, a_send.at[i], a_recv.at[i], near_y if i == 1 else near_x).wait_recv()

    def over(i, side):
        ref = windows.at[group(i) + (side,)]
        return remote(ref, ref, p_send.at[i], p_recv.at[i], partner)

    def turn(i):
        yy, xx = group(i)
        for side in range(2):
            tall = windows[yy, xx, side].T
            at = pl.multiple_of(((yy * 2 + xx) * 2 + side) * LANES, LANES)
            for k in range(2):
                left[k, :, pl.ds(at, LANES)] = tall[k * rows:(k + 1) * rows]

    def line_ref(u, source):
        return held[u].at[:, :, source] if is_early(units[u][0]) else held[u].at[y, :, source]

    def line(u, source, way, to):
        ref = line_ref(u, source)
        return remote(ref, ref, z_send.at[u, source, way], z_recv.at[u, source], (t, to, core))

    def own_lines(u, act):
        for way, (there, to) in enumerate(((z > 0, z - 1), (z < depth - 1, z + 1)) + ends):
            @pl.when(there)
            def _():
                act(line(u, z, min(way, 2), to))

    def forward(u, off, act):
        if abs(off) + 2 < depth:
            @pl.when((z > 0) if off > 0 else (z < depth - 1))
            def _():
                act(line(u, z + off, int(off < 0), z - 1 if off > 0 else z + 1))

    def there(off):
        return (z + off >= 0) & (z + off < depth)

    def line_step(u, off):
        @pl.when(there(off))
        def _():
            line(u, z + off, 2, z).wait_recv()
            forward(u, off, lambda c: c.start())
            if not is_early(units[u][0]):
                to_y(u, z + off, y).start()

    def own_step(u):
        if is_early(units[u][0]):
            to_y(u, z, 1 - y).wait_recv()
            own_lines(u, lambda c: c.start())
        else:
            swap_wait(u)
            own_lines(u, lambda c: c.start())
            to_y(u, z, y).start()

    def out(u, side):
        dst = o_ref.at[:, pl.ds(columns_of(u, side), units[u][1] * LANES)]
        return remote(ship[u], dst, out_send.at[u], out_recv.at[u], near_x)

    def term(u, side):
        block = [held[u][:, :, :, j].reshape(-1, LANES) for j in range(units[u][1])]
        wide = block[0] if len(block) == 1 else jnp.concatenate(block, axis=1)
        return jnp.dot(left[side], wide, preferred_element_type=jnp.float32).astype(o_ref.dtype)

    def multiply(u):
        form, n = units[u]
        if not is_early(form):
            for source in range(depth):
                to_y(u, source, 1 - y).wait_recv()
        if not is_whole(form):
            ship[u][...] = term(u, 1 - x)
        o_ref[:, pl.ds(columns_of(u, x), n * LANES)] = term(u, x)
        if not is_whole(form):
            out(u, x).start()

    for act in order:
        what, rest = act[0], act[1:]
        if what == SWAP:
            u = rest[0]
            for j in range(units[u][1]):
                (own_in if give[u] is None else give_in)(u, j).wait()
            swap(u).start()
        elif what == A_NEAR_Y:
            a_in(1).wait()
            a_out(1).start()
        elif what == A_NEAR_X:
            a_in(0).wait()
            over(3, core).start()

            @pl.when(core == 1)
            def _():
                a_out(0).start()
        elif what == A_OTHER_X:
            @pl.when(core == 1)
            def _():
                over(3, 0).wait_recv()
                a_out(3).start()
        elif what == A_ON:
            a_wait(1)
            a_out(2).start()
            over(1, core).start()
        elif what == A_TAKE:
            @pl.when(core == 1)
            def _():
                a_wait(0)
                over(0, 1).start()
                a_wait(3)
                over(4, 0).start()
        elif what == TURN_MOST:
            @pl.when(core == 0)
            def _():
                over(3, 1).wait_recv()

            turn(3)
            over(1, 1 - core).wait_recv()
            turn(1)

            @pl.when(core == 0)
            def _():
                over(0, 1).wait_recv()
                over(4, 0).wait_recv()

            turn(0)
        elif what == A_LAST:
            a_wait(2)
            over(2, core).start()
        elif what == TURN_LAST:
            over(2, 1 - core).wait_recv()
            turn(2)
        elif what == TO_Y:
            u = rest[0]
            swap_wait(u)
            to_y(u, z, y).start()
        elif what == OWN:
            own_step(*rest)
        elif what == LINE:
            line_step(*rest)
        elif what == MULTIPLY:
            multiply(*rest)

    for i in (1, 2):
        a_out(i).wait_send()
    for i in (1, 2, 3):
        over(i, core).wait_send()

    @pl.when(core == 1)
    def _():
        for i in (0, 3):
            a_out(i).wait_send()
        over(0, 1).wait_send()
        over(4, 0).wait_send()

    for u, (form, _) in enumerate(units):
        swap(u).wait_send()
        own_lines(u, lambda c: c.wait_send())
        to_y(u, z, y).wait_send()
        for off in range(1 - depth, depth):
            if off:
                @pl.when(there(off))
                def _():
                    forward(u, off, lambda c: c.wait_send())
                    if not is_early(form):
                        to_y(u, z + off, y).wait_send()
        if not is_whole(form):
            out(u, x).wait_send()
            out(u, 1 - x).wait_recv()


def gathered(shape, inputs, out_grad):
    depth = shape["din"]
    groups = shape["tok"]
    rows = inputs.shape[1] // groups
    piece = inputs.shape[0]
    tall, columns = out_grad.shape
    units, order = plan(columns // LANES, depth)
    count = len(units)
    most = max(n for _, n in units)
    tokens = tall * depth * groups
    kind = out_grad.dtype
    dma = pltpu.SemaphoreType.DMA
    return pl.pallas_call(
        functools.partial(kernel, (depth, rows, units, order)),
        out_shape=jax.ShapeDtypeStruct((rows, columns), kind),
        in_specs=[pl.BlockSpec(memory_space=pltpu.HBM)] * 2,
        out_specs=pl.BlockSpec(memory_space=pltpu.VMEM),
        scratch_shapes=[
            *[pltpu.VMEM((2, 2, depth, n, tall, LANES), kind) for _, n in units],
            *[pltpu.VMEM((n, tall, LANES), kind) for form, n in units if not is_whole(form)],
            *[pltpu.VMEM((rows, n * LANES), kind) for form, n in units if not is_whole(form)],
            pltpu.VMEM((piece, 2 * rows), kind),
            pltpu.VMEM((2, 2, 2, piece, 2 * rows), kind),
            pltpu.VMEM((2, rows, tokens), kind),
            dma((count, most)),
            dma((count, most)),
            dma((2,)),
            dma((4,)),
            dma((4,)),
            dma((5,)),
            dma((5,)),
            dma((count,)),
            dma((count,)),
            dma((count, depth)),
            dma((count, depth)),
            dma((count, depth, 3)),
            dma((count, depth)),
            dma((count,)),
            dma((count,)),
        ],
        compiler_params=pltpu.CompilerParams(
            collective_id=0, has_side_effects=True, vmem_limit_bytes=40 * 2**20
        ),
        cost_estimate=pl.CostEstimate(
            flops=2 * rows * tokens * columns,
            bytes_accessed=2 * rows * columns,
            transcendentals=0,
        ),
    )(*[pltpu.with_memory_space_constraint(v, pltpu.HBM) for v in (inputs, out_grad)])


def solution(mesh):
    shape = dict(mesh.shape)

    def local(inputs, out_grad):
        groups, depth = shape["tok"], shape["din"]
        rows = inputs.shape[1] // groups
        tall, columns = out_grad.shape
        fits = (
            groups == 4
            and shape["dout"] == 2
            and 2 < depth <= 8
            and inputs.shape[0] == LANES
            and tall * depth == 2 * LANES
            and rows % 64 == 0
            and tall % 16 == 0
            and columns % (2 * LANES) == 0
            and columns >= 16 * LANES
            and rows * columns <= 2**21
        )
        if fits:
            return gathered(shape, inputs, out_grad)
        return scattered(inputs, out_grad)

    placed = (P(("tok", "dout"), "din"), P(("tok", "din"), "dout"))
    return jax.shard_map(
        local, mesh=mesh, in_specs=placed, out_specs=P(("din", "tok"), "dout"), check_vma=False
    )
```

```python
import functools

import jax
import jax.numpy as jnp
from jax import lax
from jax.experimental import pallas as pl
from jax.experimental.pallas import tpu as pltpu
from jax.sharding import PartitionSpec as P

MESH = pl.DeviceIdType.MESH
LANES = 128
SPLIT, SPLIT_EARLY, WHOLE, WHOLE_EARLY = range(4)
SWAP, A_NEAR_Y, A_NEAR_X, A_ON, A_TAKE, TURN_MOST, A_LAST, TURN_LAST, TO_Y, OWN, LINE, MULTIPLY, A_OTHER_X = range(13)
UNITS = [(SPLIT, 1), (SPLIT, 1), (SPLIT, 2), (SPLIT, 2), (SPLIT, 2), (WHOLE, 2), (SPLIT, 2), (WHOLE_EARLY, 2), (SPLIT, 2), (SPLIT_EARLY, 2), (SPLIT, 2)]
ORDER = [
    (1,), (0, 8), (0, 10), (0, 9), (0, 6), (2,), (12,), (9, 8), (9, 10),
    (10, 8, 1), (10, 8, -1), (0, 4), (9, 6), (3,), (8, 9), (10, 8, -2), (10, 8, 3), (0, 0),
    (10, 8, -3), (4,), (10, 8, 2), (10, 10, -1), (10, 10, 1), (5,), (9, 4), (0, 7), (0, 5),
    (6,), (0, 1), (10, 10, 3), (0, 2), (10, 10, -3), (10, 10, 2), (10, 10, -2), (10, 6, 1), (0, 3),
    (10, 6, -1), (9, 0), (10, 6, 3), (7,), (9, 9), (11, 8), (10, 6, -2), (10, 6, -3), (11, 10),
    (10, 6, 2), (10, 0, 1), (10, 0, -1), (10, 0, 3), (10, 4, -1), (10, 4, 1), (10, 9, 1), (10, 0, -3), (10, 0, -2),
    (10, 0, 2), (10, 9, -1), (10, 4, -3), (9, 2), (11, 6), (10, 4, -2), (10, 4, 2), (10, 4, 3), (8, 7),
    (11, 0), (10, 9, 3), (9, 3), (11, 4), (10, 9, 2), (10, 2, 1), (10, 2, -3), (10, 2, -1), (10, 2, 3),
    (10, 9, -3), (9, 1), (10, 3, 3), (10, 9, -2), (11, 9), (10, 3, -1), (10, 2, 2), (10, 2, -2), (10, 3, -3),
    (10, 3, 1), (9, 5), (10, 1, -1), (10, 3, -2), (11, 2), (10, 3, 2), (10, 1, 1), (10, 1, -3), (10, 1, -2),
    (9, 7), (10, 5, -1), (10, 5, 1), (10, 1, 3), (10, 5, 3), (10, 1, 2), (11, 3), (10, 7, 1), (10, 5, -3),
    (10, 5, -2), (10, 5, 2), (10, 7, -1), (11, 1), (11, 5), (10, 7, -2), (10, 7, 2), (10, 7, 3), (10, 7, -3),
    (11, 7),
]


def scattered(inputs, out_grad):
    gathered = lax.all_gather(inputs, "dout", axis=0, tiled=True)
    partial_term = lax.dot_general(
        gathered,
        lax.all_gather(out_grad, "din", axis=0, tiled=True),
        (((0,), (0,)), ((), ())),
        preferred_element_type=jnp.float32,
    )
    return lax.psum_scatter(
        partial_term.astype(jnp.bfloat16), "tok", scatter_dimension=0, tiled=True
    )


def plan(strips, depth):
    if depth == 4 and sum(n * (1 if is_whole(form) else 2) for form, n in UNITS) == strips:
        return UNITS, ORDER
    units = [(SPLIT, 2)] * (strips // 4) + [(WHOLE, 2)] * (strips % 4 // 2)
    return units, plain_order(units, depth)


def is_whole(form):
    return form >= WHOLE


def is_early(form):
    return form % 2 == 1


def plain_order(units, depth):
    reach = depth - 1
    split = [u for u, (form, _) in enumerate(units) if not is_whole(form)]
    acts = [(SWAP, split[0]), (A_NEAR_Y,)] + [(SWAP, u) for u in split[1:5]] + [(A_NEAR_X,), (A_OTHER_X,)]
    acts += [(SWAP, u) for u in range(len(units)) if u not in split] + [(SWAP, u) for u in split[5:]]
    for s in range(len(units) + reach):
        if s < len(units):
            acts += [(TO_Y, s)] if is_early(units[s][0]) else []
            acts.append((OWN, s))
        for hop in range(reach - 1, 0, -1):
            if 0 <= s - hop < len(units):
                acts += [(LINE, s - hop, -hop), (LINE, s - hop, hop)]
                if hop == reach - 1:
                    acts += [(LINE, s - hop, -reach), (LINE, s - hop, reach)]
        if s == 1:
            acts += [(A_ON,)]
        if s == 2:
            acts += [(A_TAKE,), (TURN_MOST,), (A_LAST,), (TURN_LAST,)]
        if s >= reach:
            acts.append((MULTIPLY, s - reach))
    return acts


def kernel(sizes, a_ref, g_ref, o_ref, *scratch):
    depth, rows, units, order = sizes
    count = len(units)
    scratch = list(scratch)
    held = [scratch.pop(0) for _ in units]
    give = [None if is_whole(form) else scratch.pop(0) for form, _ in units]
    ship = [None if is_whole(form) else scratch.pop(0) for form, _ in units]
    (away, windows, left, own_load, give_load, a_load, a_send, a_recv, p_send, p_recv,
     x_send, x_recv, y_send, y_recv, z_send, z_recv, out_send, out_recv) = scratch
    t, z, core = lax.axis_index("tok"), lax.axis_index("din"), lax.axis_index("dout")
    y, x = t // 2, t % 2
    near_x = (y * 2 + (1 - x), z, core)
    near_y = ((1 - y) * 2 + x, z, core)
    partner = (t, z, 1 - core)
    ends = ((z == 0, depth - 1), (z == depth - 1, 0))
    half = sum(n for form, n in units if not is_whole(form)) * LANES
    pair = 2 * rows
    starts = []
    for u, (form, _) in enumerate(units):
        alike = [n for other, n in units[:u] if is_whole(other) == is_whole(form)]
        starts.append(sum(alike) * LANES + (2 * half if is_whole(form) else 0))

    def columns_of(u, side):
        return starts[u] if is_whole(units[u][0]) else pl.multiple_of(side * half + starts[u], LANES)

    def strip(u, side, j):
        return g_ref.at[:, pl.ds(columns_of(u, side) + j * LANES, LANES)]

    def own_in(u, j):
        return pltpu.make_async_copy(strip(u, x, j), held[u].at[y, x, z, j], own_load.at[u, j])

    def give_in(u, j):
        return pltpu.make_async_copy(strip(u, 1 - x, j), give[u].at[j], give_load.at[u, j])

    def a_in(i):
        src = a_ref.at[:, pl.ds(pl.multiple_of((y if i == 0 else 1 - y) * pair, LANES), pair)]
        return pltpu.make_async_copy(src, windows.at[y, x, core] if i == 0 else away, a_load.at[i])

    def load(u):
        for j in range(units[u][1]):
            if give[u] is not None:
                give_in(u, j).start()
            own_in(u, j).start()

    first = next(act[1] for act in order if act[0] == SWAP)
    load(first)
    for i in (1, 0):
        a_in(i).start()
    for u in range(count):
        if u != first:
            load(u)

    barrier = pltpu.get_barrier_semaphore()
    for other in (near_x, near_y, partner):
        pl.semaphore_signal(barrier, inc=1, device_id=other, device_id_type=MESH)
    greeted = 3
    for there, to in ((z > 0, z - 1), (z < depth - 1, z + 1)) + ends:
        greeted += jnp.where(there, 1, 0)

        @pl.when(there)
        def _():
            pl.semaphore_signal(barrier, inc=1, device_id=(t, to, core), device_id_type=MESH)

    pl.semaphore_wait(barrier, greeted)

    def remote(src, dst, send, recv, device):
        return pltpu.make_async_remote_copy(
            src_ref=src, dst_ref=dst, send_sem=send, recv_sem=recv,
            device_id=device, device_id_type=MESH,
        )

    def swap(u):
        dst = held[u].at[y, x, z]
        return remote(dst if give[u] is None else give[u], dst, x_send.at[u], x_recv.at[u], near_x)

    def swap_wait(u):
        if give[u] is not None:
            for j in range(units[u][1]):
                own_in(u, j).wait()
        ref = held[u].at[y, 1 - x, z]
        remote(ref, ref, x_send.at[u], x_recv.at[u], near_x).wait_recv()

    def to_y(u, source, row):
        ref = held[u].at[row, :, source]
        return remote(ref, ref, y_send.at[u, source], y_recv.at[u, source], near_y)

    def a_out(i):
        src = (windows.at[y, x, core], away, windows.at[1 - y, x, core], windows.at[y, x, 1 - core])[i]
        dst = windows.at[y, x, core] if i == 1 else src
        return remote(src, dst, a_send.at[i], a_recv.at[i], near_y if i == 1 else near_x)

    def group(i):
        return ((y, 1 - x), (1 - y, x), (1 - y, 1 - x), (y, x), (y, 1 - x))[i]

    def a_wait(i):
        yy, xx = group(i) if i < 3 else (y, 1 - x)
        ref = windows.at[yy, xx, 1 - core if i == 3 else core]
        remote(ref, ref, a_send.at[i], a_recv.at[i], near_y if i == 1 else near_x).wait_recv()

    def over(i, side):
        ref = windows.at[group(i) + (side,)]
        return remote(ref, ref, p_send.at[i], p_recv.at[i], partner)

    def turn(i):
        yy, xx = group(i)
        for side in range(2):
            tall = windows[yy, xx, side].T
            at = pl.multiple_of(((yy * 2 + xx) * 2 + side) * LANES, LANES)
            for k in range(2):
                left[k, :, pl.ds(at, LANES)] = tall[k * rows:(k + 1) * rows]

    def line_ref(u, source):
        return held[u].at[:, :, source] if is_early(units[u][0]) else held[u].at[y, :, source]

    def line(u, source, way, to):
        ref = line_ref(u, source)
        return remote(ref, ref, z_send.at[u, source, way], z_recv.at[u, source], (t, to, core))

    def own_lines(u, act):
        for way, (there, to) in enumerate(((z > 0, z - 1), (z < depth - 1, z + 1)) + ends):
            @pl.when(there)
            def _():
                act(line(u, z, min(way, 2), to))

    def forward(u, off, act):
        if abs(off) + 2 < depth:
            @pl.when((z > 0) if off > 0 else (z < depth - 1))
            def _():
                act(line(u, z + off, int(off < 0), z - 1 if off > 0 else z + 1))

    def there(off):
        return (z + off >= 0) & (z + off < depth)

    def line_step(u, off):
        @pl.when(there(off))
        def _():
            line(u, z + off, 2, z).wait_recv()
            forward(u, off, lambda c: c.start())
            if not is_early(units[u][0]):
                to_y(u, z + off, y).start()

    def own_step(u):
        if is_early(units[u][0]):
            to_y(u, z, 1 - y).wait_recv()
            own_lines(u, lambda c: c.start())
        else:
            swap_wait(u)
            own_lines(u, lambda c: c.start())
            to_y(u, z, y).start()

    def out(u, side):
        dst = o_ref.at[:, pl.ds(columns_of(u, side), units[u][1] * LANES)]
        return remote(ship[u], dst, out_send.at[u], out_recv.at[u], near_x)

    def term(u, side):
        block = [held[u][:, :, :, j].reshape(-1, LANES) for j in range(units[u][1])]
        wide = block[0] if len(block) == 1 else jnp.concatenate(block, axis=1)
        return jnp.dot(left[side], wide, preferred_element_type=jnp.float32).astype(o_ref.dtype)

    def multiply(u):
        form, n = units[u]
        if not is_early(form):
            for source in range(depth):
                to_y(u, source, 1 - y).wait_recv()
        if not is_whole(form):
            ship[u][...] = term(u, 1 - x)
        o_ref[:, pl.ds(columns_of(u, x), n * LANES)] = term(u, x)
        if not is_whole(form):
            out(u, x).start()

    for act in order:
        what, rest = act[0], act[1:]
        if what == SWAP:
            u = rest[0]
            for j in range(units[u][1]):
                (own_in if give[u] is None else give_in)(u, j).wait()
            swap(u).start()
        elif what == A_NEAR_Y:
            a_in(1).wait()
            a_out(1).start()
        elif what == A_NEAR_X:
            a_in(0).wait()
            over(3, core).start()

            @pl.when(core == 1)
            def _():
                a_out(0).start()
        elif what == A_OTHER_X:
            @pl.when(core == 1)
            def _():
                over(3, 0).wait_recv()
                a_out(3).start()
        elif what == A_ON:
            a_wait(1)
            a_out(2).start()
            over(1, core).start()
        elif what == A_TAKE:
            @pl.when(core == 1)
            def _():
                a_wait(0)
                over(0, 1).start()
                a_wait(3)
                over(4, 0).start()
        elif what == TURN_MOST:
            @pl.when(core == 0)
            def _():
                over(3, 1).wait_recv()

            turn(3)
            over(1, 1 - core).wait_recv()
            turn(1)

            @pl.when(core == 0)
            def _():
                over(0, 1).wait_recv()
                over(4, 0).wait_recv()

            turn(0)
        elif what == A_LAST:
            a_wait(2)
            over(2, core).start()
        elif what == TURN_LAST:
            over(2, 1 - core).wait_recv()
            turn(2)
        elif what == TO_Y:
            u = rest[0]
            swap_wait(u)
            to_y(u, z, y).start()
        elif what == OWN:
            own_step(*rest)
        elif what == LINE:
            line_step(*rest)
        elif what == MULTIPLY:
            multiply(*rest)

    for i in (1, 2):
        a_out(i).wait_send()
    for i in (1, 2, 3):
        over(i, core).wait_send()

    @pl.when(core == 1)
    def _():
        for i in (0, 3):
            a_out(i).wait_send()
        over(0, 1).wait_send()
        over(4, 0).wait_send()

    for u, (form, _) in enumerate(units):
        swap(u).wait_send()
        own_lines(u, lambda c: c.wait_send())
        to_y(u, z, y).wait_send()
        for off in range(1 - depth, depth):
            if off:
                @pl.when(there(off))
                def _():
                    forward(u, off, lambda c: c.wait_send())
                    if not is_early(form):
                        to_y(u, z + off, y).wait_send()
        if not is_whole(form):
            out(u, x).wait_send()
            out(u, 1 - x).wait_recv()


def gathered(shape, inputs, out_grad):
    depth = shape["din"]
    groups = shape["tok"]
    rows = inputs.shape[1] // groups
    piece = inputs.shape[0]
    tall, columns = out_grad.shape
    units, order = plan(columns // LANES, depth)
    count = len(units)
    most = max(n for _, n in units)
    tokens = tall * depth * groups
    kind = out_grad.dtype
    dma = pltpu.SemaphoreType.DMA
    return pl.pallas_call(
        functools.partial(kernel, (depth, rows, units, order)),
        out_shape=jax.ShapeDtypeStruct((rows, columns), kind),
        in_specs=[pl.BlockSpec(memory_space=pltpu.HBM)] * 2,
        out_specs=pl.BlockSpec(memory_space=pltpu.VMEM),
        scratch_shapes=[
            *[pltpu.VMEM((2, 2, depth, n, tall, LANES), kind) for _, n in units],
            *[pltpu.VMEM((n, tall, LANES), kind) for form, n in units if not is_whole(form)],
            *[pltpu.VMEM((rows, n * LANES), kind) for form, n in units if not is_whole(form)],
            pltpu.VMEM((piece, 2 * rows), kind),
            pltpu.VMEM((2, 2, 2, piece, 2 * rows), kind),
            pltpu.VMEM((2, rows, tokens), kind),
            dma((count, most)),
            dma((count, most)),
            dma((2,)),
            dma((4,)),
            dma((4,)),
            dma((5,)),
            dma((5,)),
            dma((count,)),
            dma((count,)),
            dma((count, depth)),
            dma((count, depth)),
            dma((count, depth, 3)),
            dma((count, depth)),
            dma((count,)),
            dma((count,)),
        ],
        compiler_params=pltpu.CompilerParams(
            collective_id=0, has_side_effects=True, vmem_limit_bytes=40 * 2**20
        ),
        cost_estimate=pl.CostEstimate(
            flops=2 * rows * tokens * columns,
            bytes_accessed=2 * rows * columns,
            transcendentals=0,
        ),
    )(*[pltpu.with_memory_space_constraint(v, pltpu.HBM) for v in (inputs, out_grad)])


def solution(mesh):
    shape = dict(mesh.shape)

    def local(inputs, out_grad):
        groups, depth = shape["tok"], shape["din"]
        rows = inputs.shape[1] // groups
        tall, columns = out_grad.shape
        fits = (
            groups == 4
            and shape["dout"] == 2
            and 2 < depth <= 8
            and inputs.shape[0] == LANES
            and tall * depth == 2 * LANES
            and rows % 64 == 0
            and tall % 16 == 0
            and columns % (2 * LANES) == 0
            and columns >= 16 * LANES
            and rows * columns <= 2**21
        )
        if fits:
            return gathered(shape, inputs, out_grad)
        return scattered(inputs, out_grad)

    placed = (P(("tok", "dout"), "din"), P(("tok", "din"), "dout"))
    return jax.shard_map(
        local, mesh=mesh, in_specs=placed, out_specs=P(("din", "tok"), "dout"), check_vma=False
    )
```

```python
import functools

import jax
import jax.numpy as jnp
from jax import lax
from jax.experimental import pallas as pl
from jax.experimental.pallas import tpu as pltpu
from jax.sharding import PartitionSpec as P

MESH = pl.DeviceIdType.MESH
LANES = 128
SPLIT, SPLIT_EARLY, WHOLE, WHOLE_EARLY = range(4)
SWAP, A_NEAR_Y, A_NEAR_X, A_ON, A_TAKE, TURN_MOST, A_LAST, TURN_LAST, TO_Y, OWN, LINE, MULTIPLY, A_OTHER_X = range(13)
UNITS = [(SPLIT, 1), (SPLIT, 1), (SPLIT, 2), (SPLIT, 2), (SPLIT, 2), (WHOLE, 2), (SPLIT, 2), (WHOLE_EARLY, 2), (SPLIT, 2), (SPLIT_EARLY, 2), (SPLIT, 2)]
ORDER = [
    (1,), (0, 8), (0, 10), (0, 9), (0, 6), (2,), (12,), (9, 8), (9, 10),
    (10, 8, 1), (10, 8, -1), (0, 4), (9, 6), (3,), (8, 9), (10, 8, -2), (10, 8, 3), (0, 0),
    (10, 8, -3), (4,), (10, 8, 2), (10, 10, -1), (10, 10, 1), (5,), (9, 4), (0, 7), (0, 5),
    (6,), (0, 1), (10, 10, 3), (0, 2), (10, 10, -3), (10, 10, 2), (10, 10, -2), (10, 6, 1), (0, 3),
    (10, 6, -1), (9, 0), (10, 6, 3), (7,), (9, 9), (11, 8), (10, 6, -2), (10, 6, -3), (11, 10),
    (10, 6, 2), (10, 0, 1), (10, 0, -1), (10, 0, 3), (10, 4, -1), (10, 4, 1), (10, 9, 1), (10, 0, -3), (10, 0, -2),
    (10, 0, 2), (10, 9, -1), (10, 4, -3), (9, 2), (11, 6), (10, 4, -2), (10, 4, 2), (10, 4, 3), (8, 7),
    (11, 0), (10, 9, 3), (9, 3), (11, 4), (10, 9, 2), (10, 2, 1), (10, 2, -3), (10, 2, -1), (10, 2, 3),
    (10, 9, -3), (9, 1), (10, 3, 3), (10, 9, -2), (11, 9), (10, 3, -1), (10, 2, 2), (10, 2, -2), (10, 3, -3),
    (10, 3, 1), (9, 5), (10, 1, -1), (10, 3, -2), (11, 2), (10, 3, 2), (10, 1, 1), (10, 1, -3), (10, 1, -2),
    (9, 7), (10, 5, -1), (10, 5, 1), (10, 1, 3), (10, 5, 3), (10, 1, 2), (11, 3), (10, 7, 1), (10, 5, -3),
    (10, 5, -2), (10, 5, 2), (10, 7, -1), (11, 1), (11, 5), (10, 7, -2), (10, 7, 2), (10, 7, 3), (10, 7, -3),
    (11, 7),
]


def scattered(inputs, out_grad):
    gathered = lax.all_gather(inputs, "dout", axis=0, tiled=True)
    partial_term = lax.dot_general(
        gathered,
        lax.all_gather(out_grad, "din", axis=0, tiled=True),
        (((0,), (0,)), ((), ())),
        preferred_element_type=jnp.float32,
    )
    return lax.psum_scatter(
        partial_term.astype(jnp.bfloat16), "tok", scatter_dimension=0, tiled=True
    )


def plan(strips, depth):
    if depth == 4 and sum(n * (1 if is_whole(form) else 2) for form, n in UNITS) == strips:
        return UNITS, ORDER
    units = [(SPLIT, 2)] * (strips // 4) + [(WHOLE, 2)] * (strips % 4 // 2)
    return units, plain_order(units, depth)


def is_whole(form):
    return form >= WHOLE


def is_early(form):
    return form % 2 == 1


def plain_order(units, depth):
    reach = depth - 1
    split = [u for u, (form, _) in enumerate(units) if not is_whole(form)]
    acts = [(SWAP, split[0]), (A_NEAR_Y,)] + [(SWAP, u) for u in split[1:5]] + [(A_NEAR_X,), (A_OTHER_X,)]
    acts += [(SWAP, u) for u in range(len(units)) if u not in split] + [(SWAP, u) for u in split[5:]]
    for s in range(len(units) + reach):
        if s < len(units):
            acts += [(TO_Y, s)] if is_early(units[s][0]) else []
            acts.append((OWN, s))
        for hop in range(reach - 1, 0, -1):
            if 0 <= s - hop < len(units):
                acts += [(LINE, s - hop, -hop), (LINE, s - hop, hop)]
                if hop == reach - 1:
                    acts += [(LINE, s - hop, -reach), (LINE, s - hop, reach)]
        if s == 1:
            acts += [(A_ON,)]
        if s == 2:
            acts += [(A_TAKE,), (TURN_MOST,), (A_LAST,), (TURN_LAST,)]
        if s >= reach:
            acts.append((MULTIPLY, s - reach))
    return acts


def kernel(sizes, a_ref, g_ref, o_ref, *scratch):
    depth, rows, units, order = sizes
    count = len(units)
    scratch = list(scratch)
    held = [scratch.pop(0) for _ in units]
    give = [None if is_whole(form) else scratch.pop(0) for form, _ in units]
    ship = [None if is_whole(form) else scratch.pop(0) for form, _ in units]
    (away, windows, left, own_load, give_load, a_load, a_send, a_recv, p_send, p_recv,
     x_send, x_recv, y_send, y_recv, z_send, z_recv, out_send, out_recv) = scratch
    t, z, core = lax.axis_index("tok"), lax.axis_index("din"), lax.axis_index("dout")
    y, x = t // 2, t % 2
    near_x = (y * 2 + (1 - x), z, core)
    near_y = ((1 - y) * 2 + x, z, core)
    partner = (t, z, 1 - core)
    ends = ((z == 0, depth - 1), (z == depth - 1, 0))
    half = sum(n for form, n in units if not is_whole(form)) * LANES
    pair = 2 * rows
    starts = []
    for u, (form, _) in enumerate(units):
        alike = [n for other, n in units[:u] if is_whole(other) == is_whole(form)]
        starts.append(sum(alike) * LANES + (2 * half if is_whole(form) else 0))

    def columns_of(u, side):
        return starts[u] if is_whole(units[u][0]) else pl.multiple_of(side * half + starts[u], LANES)

    def strip(u, side, j):
        return g_ref.at[:, pl.ds(columns_of(u, side) + j * LANES, LANES)]

    def own_in(u, j):
        return pltpu.make_async_copy(strip(u, x, j), held[u].at[y, x, z, j], own_load.at[u, j])

    def give_in(u, j):
        return pltpu.make_async_copy(strip(u, 1 - x, j), give[u].at[j], give_load.at[u, j])

    def a_in(i):
        src = a_ref.at[:, pl.ds(pl.multiple_of((y if i == 0 else 1 - y) * pair, LANES), pair)]
        return pltpu.make_async_copy(src, windows.at[y, x, core] if i == 0 else away, a_load.at[i])

    def load(u):
        for j in range(units[u][1]):
            if give[u] is not None:
                give_in(u, j).start()
            own_in(u, j).start()

    first = next(act[1] for act in order if act[0] == SWAP)
    load(first)
    for i in (1, 0):
        a_in(i).start()
    for u in range(count):
        if u != first:
            load(u)

    barrier = pltpu.get_barrier_semaphore()
    for other in (near_x, near_y, partner):
        pl.semaphore_signal(barrier, inc=1, device_id=other, device_id_type=MESH)
    greeted = 3
    for there, to in ((z > 0, z - 1), (z < depth - 1, z + 1)) + ends:
        greeted += jnp.where(there, 1, 0)

        @pl.when(there)
        def _():
            pl.semaphore_signal(barrier, inc=1, device_id=(t, to, core), device_id_type=MESH)

    pl.semaphore_wait(barrier, greeted)

    def remote(src, dst, send, recv, device):
        return pltpu.make_async_remote_copy(
            src_ref=src, dst_ref=dst, send_sem=send, recv_sem=recv,
            device_id=device, device_id_type=MESH,
        )

    def swap(u):
        dst = held[u].at[y, x, z]
        return remote(dst if give[u] is None else give[u], dst, x_send.at[u], x_recv.at[u], near_x)

    def swap_wait(u):
        if give[u] is not None:
            for j in range(units[u][1]):
                own_in(u, j).wait()
        ref = held[u].at[y, 1 - x, z]
        remote(ref, ref, x_send.at[u], x_recv.at[u], near_x).wait_recv()

    def to_y(u, source, row):
        ref = held[u].at[row, :, source]
        return remote(ref, ref, y_send.at[u, source], y_recv.at[u, source], near_y)

    def a_out(i):
        src = (windows.at[y, x, core], away, windows.at[1 - y, x, core], windows.at[y, x, 1 - core])[i]
        dst = windows.at[y, x, core] if i == 1 else src
        return remote(src, dst, a_send.at[i], a_recv.at[i], near_y if i == 1 else near_x)

    def group(i):
        return ((y, 1 - x), (1 - y, x), (1 - y, 1 - x), (y, x), (y, 1 - x))[i]

    def a_wait(i):
        yy, xx = group(i) if i < 3 else (y, 1 - x)
        ref = windows.at[yy, xx, 1 - core if i == 3 else core]
        remote(ref, ref, a_send.at[i], a_recv.at[i], near_y if i == 1 else near_x).wait_recv()

    def over(i, side):
        ref = windows.at[group(i) + (side,)]
        return remote(ref, ref, p_send.at[i], p_recv.at[i], partner)

    def turn(i):
        yy, xx = group(i)
        for side in range(2):
            tall = windows[yy, xx, side].T
            at = pl.multiple_of(((yy * 2 + xx) * 2 + side) * LANES, LANES)
            for k in range(2):
                left[k, :, pl.ds(at, LANES)] = tall[k * rows:(k + 1) * rows]

    def line_ref(u, source):
        return held[u].at[:, :, source] if is_early(units[u][0]) else held[u].at[y, :, source]

    def line(u, source, way, to):
        ref = line_ref(u, source)
        return remote(ref, ref, z_send.at[u, source, way], z_recv.at[u, source], (t, to, core))

    def own_lines(u, act):
        for way, (there, to) in enumerate(((z > 0, z - 1), (z < depth - 1, z + 1)) + ends):
            @pl.when(there)
            def _():
                act(line(u, z, min(way, 2), to))

    def forward(u, off, act):
        if abs(off) + 2 < depth:
            @pl.when((z > 0) if off > 0 else (z < depth - 1))
            def _():
                act(line(u, z + off, int(off < 0), z - 1 if off > 0 else z + 1))

    def there(off):
        return (z + off >= 0) & (z + off < depth)

    def line_step(u, off):
        @pl.when(there(off))
        def _():
            line(u, z + off, 2, z).wait_recv()
            forward(u, off, lambda c: c.start())
            if not is_early(units[u][0]):
                to_y(u, z + off, y).start()

    def own_step(u):
        if is_early(units[u][0]):
            to_y(u, z, 1 - y).wait_recv()
            own_lines(u, lambda c: c.start())
        else:
            swap_wait(u)
            own_lines(u, lambda c: c.start())
            to_y(u, z, y).start()

    def out(u, side):
        dst = o_ref.at[:, pl.ds(columns_of(u, side), units[u][1] * LANES)]
        return remote(ship[u], dst, out_send.at[u], out_recv.at[u], near_x)

    def term(u, side):
        block = [held[u][:, :, :, j].reshape(-1, LANES) for j in range(units[u][1])]
        wide = block[0] if len(block) == 1 else jnp.concatenate(block, axis=1)
        return jnp.dot(left[side], wide, preferred_element_type=jnp.float32).astype(o_ref.dtype)

    def multiply(u):
        form, n = units[u]
        if not is_early(form):
            for source in range(depth):
                to_y(u, source, 1 - y).wait_recv()
        if not is_whole(form):
            ship[u][...] = term(u, 1 - x)
        o_ref[:, pl.ds(columns_of(u, x), n * LANES)] = term(u, x)
        if not is_whole(form):
            out(u, x).start()

    for act in order:
        what, rest = act[0], act[1:]
        if what == SWAP:
            u = rest[0]
            for j in range(units[u][1]):
                (own_in if give[u] is None else give_in)(u, j).wait()
            swap(u).start()
        elif what == A_NEAR_Y:
            a_in(1).wait()
            a_out(1).start()
        elif what == A_NEAR_X:
            a_in(0).wait()
            over(3, core).start()

            @pl.when(core == 1)
            def _():
                a_out(0).start()
        elif what == A_OTHER_X:
            @pl.when(core == 1)
            def _():
                over(3, 0).wait_recv()
                a_out(3).start()
        elif what == A_ON:
            a_wait(1)
            a_out(2).start()
            over(1, core).start()
        elif what == A_TAKE:
            @pl.when(core == 1)
            def _():
                a_wait(0)
                over(0, 1).start()
                a_wait(3)
                over(4, 0).start()
        elif what == TURN_MOST:
            @pl.when(core == 0)
            def _():
                over(3, 1).wait_recv()

            turn(3)
            over(1, 1 - core).wait_recv()
            turn(1)

            @pl.when(core == 0)
            def _():
                over(0, 1).wait_recv()
                over(4, 0).wait_recv()

            turn(0)
        elif what == A_LAST:
            a_wait(2)
            over(2, core).start()
        elif what == TURN_LAST:
            over(2, 1 - core).wait_recv()
            turn(2)
        elif what == TO_Y:
            u = rest[0]
            swap_wait(u)
            to_y(u, z, y).start()
        elif what == OWN:
            own_step(*rest)
        elif what == LINE:
            line_step(*rest)
        elif what == MULTIPLY:
            multiply(*rest)

    for i in (1, 2):
        a_out(i).wait_send()
    for i in (1, 2, 3):
        over(i, core).wait_send()

    @pl.when(core == 1)
    def _():
        for i in (0, 3):
            a_out(i).wait_send()
        over(0, 1).wait_send()
        over(4, 0).wait_send()

    for u, (form, _) in enumerate(units):
        swap(u).wait_send()
        own_lines(u, lambda c: c.wait_send())
        to_y(u, z, y).wait_send()
        for off in range(1 - depth, depth):
            if off:
                @pl.when(there(off))
                def _():
                    forward(u, off, lambda c: c.wait_send())
                    if not is_early(form):
                        to_y(u, z + off, y).wait_send()
        if not is_whole(form):
            out(u, x).wait_send()
            out(u, 1 - x).wait_recv()


def put_out(pieces, src, dst, sems):
    rows = src.shape[0] // pieces
    copies = [
        pltpu.make_async_copy(src.at[pl.ds(i * rows, rows)], dst.at[pl.ds(i * rows, rows)], sems.at[i])
        for i in range(pieces)
    ]
    for copy in copies:
        copy.start()
    for copy in copies:
        copy.wait()


def gathered(shape, inputs, out_grad):
    depth = shape["din"]
    groups = shape["tok"]
    rows = inputs.shape[1] // groups
    piece = inputs.shape[0]
    tall, columns = out_grad.shape
    units, order = plan(columns // LANES, depth)
    count = len(units)
    most = max(n for _, n in units)
    tokens = tall * depth * groups
    kind = out_grad.dtype
    dma = pltpu.SemaphoreType.DMA
    made = pl.pallas_call(
        functools.partial(kernel, (depth, rows, units, order)),
        out_shape=jax.ShapeDtypeStruct((rows, columns), kind),
        in_specs=[pl.BlockSpec(memory_space=pltpu.HBM)] * 2,
        out_specs=pl.BlockSpec(memory_space=pltpu.VMEM),
        scratch_shapes=[
            *[pltpu.VMEM((2, 2, depth, n, tall, LANES), kind) for _, n in units],
            *[pltpu.VMEM((n, tall, LANES), kind) for form, n in units if not is_whole(form)],
            *[pltpu.VMEM((rows, n * LANES), kind) for form, n in units if not is_whole(form)],
            pltpu.VMEM((piece, 2 * rows), kind),
            pltpu.VMEM((2, 2, 2, piece, 2 * rows), kind),
            pltpu.VMEM((2, rows, tokens), kind),
            dma((count, most)),
            dma((count, most)),
            dma((2,)),
            dma((4,)),
            dma((4,)),
            dma((5,)),
            dma((5,)),
            dma((count,)),
            dma((count,)),
            dma((count, depth)),
            dma((count, depth)),
            dma((count, depth, 3)),
            dma((count, depth)),
            dma((count,)),
            dma((count,)),
        ],
        compiler_params=pltpu.CompilerParams(
            collective_id=0, has_side_effects=True, vmem_limit_bytes=40 * 2**20
        ),
        cost_estimate=pl.CostEstimate(
            flops=2 * rows * tokens * columns,
            bytes_accessed=2 * rows * columns,
            transcendentals=0,
        ),
    )(*[pltpu.with_memory_space_constraint(v, pltpu.HBM) for v in (inputs, out_grad)])
    pieces = rows // 64
    return pl.pallas_call(
        functools.partial(put_out, pieces),
        out_shape=jax.ShapeDtypeStruct((rows, columns), kind),
        in_specs=[pl.BlockSpec(memory_space=pltpu.VMEM)],
        out_specs=pl.BlockSpec(memory_space=pltpu.HBM),
        scratch_shapes=[dma((pieces,))],
        compiler_params=pltpu.CompilerParams(vmem_limit_bytes=2**20),
    )(made)


def solution(mesh):
    shape = dict(mesh.shape)

    def local(inputs, out_grad):
        groups, depth = shape["tok"], shape["din"]
        rows = inputs.shape[1] // groups
        tall, columns = out_grad.shape
        fits = (
            groups == 4
            and shape["dout"] == 2
            and 2 < depth <= 8
            and inputs.shape[0] == LANES
            and tall * depth == 2 * LANES
            and rows % 64 == 0
            and tall % 16 == 0
            and columns % (2 * LANES) == 0
            and columns >= 16 * LANES
            and rows * columns <= 2**21
        )
        if fits:
            return gathered(shape, inputs, out_grad)
        return scattered(inputs, out_grad)

    placed = (P(("tok", "dout"), "din"), P(("tok", "din"), "dout"))
    return jax.shard_map(
        local, mesh=mesh, in_specs=placed, out_specs=P(("din", "tok"), "dout"), check_vma=False
    )
```
